64 devices in a mesh: rep: 8 (over x, y, core), dp: 8 (over z).
Axes of the slice: x: 2, y: 2, z: 8, core: 2. Of those that a mesh axis runs over, the one named last changes fastest.
The devices are a block of a 4x4x8 slice.
Arguments:
- x: bfloat16 [64, 2048, 512], P(('rep', 'dp')), parts along dimension 0
- dy: bfloat16 [64, 2048, 512], P(('rep', 'dp')), parts along dimension 0
- w_gate: bfloat16 [2, 512, 2048], P(None, 'dp')
- w_up: bfloat16 [2, 512, 2048], P(None, 'dp')
- w_down: bfloat16 [2, 2048, 512], P(None, 'dp')
Outputs:
- output 1: bfloat16 [64, 2048, 512], P(('rep', 'dp')), parts along dimension 0
- output 2: bfloat16 [16, 512, 2048], P('rep', 'dp'), parts along dimension 0
- output 3: bfloat16 [16, 512, 2048], P('rep', 'dp'), parts along dimension 0
- output 4: bfloat16 [16, 2048, 512], P('rep', 'dp'), parts along dimension 0
There are 8 independent parts. The reference program is written for one: setup_inputs(seed, part) draws one part's arguments, and reference() takes and returns one part's arrays. A program takes and returns all parts, laid end to end along the dimension named above; an argument that names none is the same for every part.
All inputs are finite; a program needn't handle non-finite values.
Results may differ from the reference program's by a relative error of at most 0.018.
Values are sent between devices in bfloat16 or wider.
A program may use at most 768 MiB of HBM per device.

```python
import jax
import jax.numpy as jnp
from jax import lax

SEQUENCES = 8
TOKENS = 2048
D = 512
FF = 2048
LAYERS = 2
NAMES = ("w_gate", "w_up", "w_down")
SHAPES = {"w_gate": (LAYERS, D, FF), "w_up": (LAYERS, D, FF), "w_down": (LAYERS, FF, D)}


def bump(key, n, height):
    away = (jnp.arange(n, dtype=jnp.int32) - jax.random.randint(key, (), 0, n, jnp.int32)) % n
    return jnp.where(away < n // 8, height, 1.0)


def together(key, own, strength):
    shared = jax.random.normal(key, own.shape[1:], jnp.float32)
    return (own + strength * shared) * lax.rsqrt(1 + strength * strength)


def setup_inputs(seed: int = 0, part: int = 0) -> dict:
    kx, kdy, ka, kb, kz, kf, kh, kl, *kw = jax.random.split(jax.random.key(seed), 8 + len(NAMES))
    kx, kdy, ka, kb = (jax.random.fold_in(k, part) for k in (kx, kdy, ka, kb))
    shape = (SEQUENCES, TOKENS, D)
    much_x, much_dy = jax.random.uniform(kz, (2,), jnp.float32, 0.0, 1.0)
    layers = 2.0 ** jax.random.uniform(kl, (LAYERS, 1, 1), jnp.float32, -1.0, 1.0)
    x = together(ka, jax.random.normal(kx, shape, jnp.float32), much_x) * bump(kf, D, 4.0)
    dy = together(kb, jax.random.normal(kdy, shape, jnp.float32), much_dy)
    drawn = {"x": x.astype(jnp.bfloat16), "dy": (dy * (SEQUENCES * TOKENS) ** -0.5).astype(jnp.bfloat16)}
    for key, name in zip(kw, NAMES, strict=True):
        w = jax.random.normal(key, SHAPES[name], jnp.float32) * SHAPES[name][1] ** -0.5
        drawn[name] = (w * {"w_gate": 1.0, "w_up": bump(kh, FF, 4.0), "w_down": layers}[name]).astype(jnp.bfloat16)
    return drawn


def matmul(a, w):
    return jnp.dot(a, w, preferred_element_type=jnp.float32).astype(jnp.bfloat16)


def normed(h):
    wide = h.astype(jnp.float32)
    scale = lax.rsqrt(jnp.mean(wide**2, -1, keepdims=True) + 1e-6)
    return (wide * scale).astype(jnp.bfloat16)


def layer(h, w):
    a = normed(h)
    gate = jnp.dot(a, w["w_gate"], preferred_element_type=jnp.float32)
    up = jnp.dot(a, w["w_up"], preferred_element_type=jnp.float32)
    return h + matmul((jax.nn.silu(gate) * up).astype(jnp.bfloat16), w["w_down"])


def stack(weights, h):
    return lax.scan(lambda h, w: (layer(h, w), None), h, weights)[0]


def reference(x, dy, w_gate, w_up, w_down):
    weights = dict(zip(NAMES, (w_gate, w_up, w_down), strict=True))

    def take(so_far, sequence):
        h, by_y = sequence
        _, back = jax.vjp(stack, weights, h)
        by_weights, by_h = back(by_y)
        return jax.tree.map(lambda total, term: total + term.astype(jnp.float32), so_far, by_weights), by_h

    none_yet = {name: jnp.zeros(w.shape, jnp.float32) for name, w in weights.items()}
    by_weights, by_x = lax.scan(take, none_yet, (x, dy))
    return (by_x, *(by_weights[name].astype(jnp.bfloat16) for name in NAMES))
```

```python
import functools

import jax
import jax.numpy as jnp
from jax import lax
from jax.experimental import pallas as pl
from jax.experimental.pallas import tpu as pltpu
from jax.sharding import PartitionSpec as P

MESH = pl.DeviceIdType.MESH
F32, BF16 = jnp.float32, jnp.bfloat16
SEGMENTS = 2
SLOTS = 5
RECV = 4
SEND = 2


def dot(a, b):
    return jnp.dot(a, b, preferred_element_type=F32)


def dot_nt(a, b):
    return lax.dot_general(a, b, (((1,), (1,)), ((), ())), preferred_element_type=F32)


def kernel(
    n, x_ref, dy_ref, wg_ref, wu_ref, wd_ref, dx_ref, dwg_ref, dwu_ref, dwd_ref,
    wgu, wdn, h, g, gt, a, at, act, dgu, da, term, sbuf, rbuf, outg, outu, outd,
    load_sem, ag_send, ag_recv, sw_send, sw_recv, rs_send, rs_recv,
):
    layers, _, d_model, ff = wgu.shape
    tokens = h.shape[1]
    rows = d_model // n
    drows = ff // n
    chunk = d_model // 2
    chunks = ff // chunk
    subs = drows // rows
    half = n // 2
    per_layer = subs + chunks
    units = layers * per_layer
    dbase = SLOTS * d_model
    seg = ff // SEGMENTS

    me, rep = lax.axis_index("dp"), lax.axis_index("rep")
    left, right = lax.rem(me + n - 1, n), lax.rem(me + 1, n)
    core = lax.rem(rep, 2)
    partner = rep + 1 - 2 * core
    toward = ({"dp": left}, {"dp": right})

    def at_distance(direction, k):
        return lax.rem(me + (n - k if direction == 0 else k), n)

    mine = pl.multiple_of(me * rows, rows)
    dmine = pl.multiple_of(me * drows, drows)
    loads = [pltpu.make_async_copy(x_ref.at[0], h.at[0], load_sem.at[0])]
    for l in range(layers):
        loads += [
            pltpu.make_async_copy(wg_ref.at[l], wgu.at[l, 0, pl.ds(mine, rows), :], load_sem.at[1 + 3 * l]),
            pltpu.make_async_copy(wu_ref.at[l], wgu.at[l, 1, pl.ds(mine, rows), :], load_sem.at[2 + 3 * l]),
            pltpu.make_async_copy(wd_ref.at[l], wdn.at[l, pl.ds(dmine, drows), :], load_sem.at[3 + 3 * l]),
        ]
    loads.append(pltpu.make_async_copy(dy_ref.at[0], g, load_sem.at[1 + 3 * layers]))
    for c in loads:
        c.start()

    barrier = pltpu.get_barrier_semaphore()
    for other in (*toward, {"rep": partner}):
        pl.semaphore_signal(barrier, inc=1, device_id=other, device_id_type=MESH)
    pl.semaphore_wait(barrier, 3)

    def piece(unit, origin, member, part=None):
        l, s = unit // (SEGMENTS + 1), unit % (SEGMENTS + 1)
        if s < SEGMENTS:
            size, first, width = rows // 2, s * seg, seg
            if part is not None:
                width = seg // 2
                first += part * width
            row = pl.multiple_of(origin * rows + member * size, size)
            return wgu.at[l, :, pl.ds(row, size), pl.ds(first, width)]
        size = drows // 2
        row = origin * drows + member * size
        if part is not None:
            size //= 2
            row += part * size
        return wdn.at[l, pl.ds(pl.multiple_of(row, size), size), :]

    def hop(unit, direction, k):
        origin = at_distance(1 - direction, k)
        ref = piece(unit, origin, core, direction if k == half - 1 else None)
        return pltpu.make_async_remote_copy(
            ref, ref, ag_send.at[unit, direction, k], ag_recv.at[unit, direction, k],
            device_id=toward[direction], device_id_type=MESH,
        )

    def landed(unit, direction, k):
        origin = at_distance(1 - direction, k + 1)
        ref = piece(unit, origin, core, direction if k == half - 1 else None)
        return pltpu.make_async_remote_copy(
            ref, ref, ag_send.at[unit, direction, k], ag_recv.at[unit, direction, k],
            device_id=toward[direction], device_id_type=MESH,
        )

    def swap(unit, direction, k, member):
        origin = at_distance(1 - direction, k + 1)
        ref = piece(unit, origin, member, direction if k == half - 1 else None)
        return pltpu.make_async_remote_copy(
            ref, ref, sw_send.at[unit, direction, k], sw_recv.at[unit, direction, k],
            device_id={"rep": partner}, device_id_type=MESH,
        )

    def gather(unit, k):
        for direction in range(2):
            if k > 0:
                landed(unit, direction, k - 1).wait_recv()
            if k < half:
                hop(unit, direction, k).start()
            if k > 0:
                swap(unit, direction, k - 1, core).start()

    def gathered(unit):
        for k in range(half):
            for direction in range(2):
                swap(unit, direction, k, 1 - core).wait_recv()

    def close(unit):
        for k in range(half):
            for direction in range(2):
                hop(unit, direction, k).wait_send()
                swap(unit, direction, k, core).wait_send()

    def place(u):
        step, v = u // per_layer, lax.rem(u, per_layer)
        l = layers - 1 - step
        mixed = 2 * subs - 1
        early = v < mixed
        down = early & ((v == 0) | (lax.rem(v, 2) == 1))
        index = jnp.where(down, (v + 1) // 2, jnp.where(early, v // 2 - 1, v - subs))
        slot = lax.rem(step * chunks + index, SLOTS)
        base = jnp.where(down, dbase + l * ff + index * rows, slot * d_model)
        stride = jnp.where(down, drows, rows)
        return l, down, index, base, stride

    def rs_copy(direction, k, u):
        lo, size = (direction * (rows // 2), rows // 2) if k == 0 else (0, rows)
        return pltpu.make_async_remote_copy(
            sbuf.at[direction, k, lax.rem(u, SEND), pl.ds(lo, size), :],
            rbuf.at[direction, k, lax.rem(u, RECV), pl.ds(lo, size), :],
            rs_send.at[direction, k, lax.rem(u, SEND)],
            rs_recv.at[direction, k, lax.rem(u, RECV)],
            device_id=toward[direction],
            device_id_type=MESH,
        )

    def stage(t, k):
        u = t - k
        l, down, index, base, stride = place(u)
        hrows = rows // 2

        def own(owner, lo, size):
            return term[pl.ds(pl.multiple_of(base + owner * stride + lo, hrows), size), :]

        if k == half:
            for direction in range(2):
                rs_copy(direction, half - 1, u).wait_recv()
            slot = lax.rem(u, RECV)
            total = own(me, 0, rows)
            for direction in range(2):
                total += rbuf[direction, half - 1, slot].astype(F32)
            total = total.astype(BF16)

            @pl.when(down)
            def _():
                outd[l, pl.ds(pl.multiple_of(index * rows, rows), rows), :] = total

            @pl.when(jnp.logical_not(down))
            def _():
                columns = pl.ds(pl.multiple_of(index * chunk, chunk), chunk)
                outg[l, :, columns] = total[:, :chunk]
                outu[l, :, columns] = total[:, chunk:]

            return
        for direction in range(2):

            @pl.when(u >= SEND)
            def _():
                rs_copy(direction, k, u - SEND).wait_send()

            owner = at_distance(direction, half - k)
            to = sbuf.at[direction, k, lax.rem(u, SEND)]
            lo = direction * hrows
            if k == 0:
                to[pl.ds(lo, hrows), :] = own(owner, lo, hrows).astype(BF16)
            else:
                rs_copy(direction, k - 1, u).wait_recv()
                came = rbuf.at[direction, k - 1, lax.rem(u, RECV)]
                if k == 1:
                    rest = hrows - lo
                    to[pl.ds(lo, hrows), :] = (own(owner, lo, hrows) + came[pl.ds(lo, hrows), :].astype(F32)).astype(BF16)
                    to[pl.ds(rest, hrows), :] = own(owner, rest, hrows).astype(BF16)
                else:
                    to[...] = (own(owner, 0, rows) + came[...].astype(F32)).astype(BF16)
            rs_copy(direction, k, u).start()

    def tick(t):
        for k in range(half + 1):
            pl.when((t >= k) & (t - k < units))(functools.partial(stage, t, k))

    small, tile = min(256, tokens), min(512, tokens)

    def normed(l):
        @pl.loop(0, tokens // small)
        def _(i):
            ts = pl.ds(pl.multiple_of(i * small, small), small)
            wide = h[l, ts, :].astype(F32)
            scale = lax.rsqrt(jnp.mean(wide * wide, -1, keepdims=True) + 1e-6)
            rounded = (wide * scale).astype(BF16)
            a[ts, :] = rounded
            at[:, ts] = rounded.T

    def turn():
        @pl.loop(0, tokens // small)
        def _(i):
            ts = pl.ds(pl.multiple_of(i * small, small), small)
            gt[:, ts] = g[ts, :].T

    def gate_up(l, ts, columns):
        rows_in = a[ts, :]
        return dot(rows_in, wgu[l, 0, :, columns]), dot(rows_in, wgu[l, 1, :, columns])

    def forward(l, s):
        tiles = tokens // tile

        @pl.loop(0, seg // chunk * tiles)
        def _(i):
            columns = pl.ds(pl.multiple_of(s * seg + i // tiles * chunk, chunk), chunk)
            ts = pl.ds(pl.multiple_of(lax.rem(i, tiles) * tile, tile), tile)
            gate, up = gate_up(l, ts, columns)
            act[ts, columns] = (gate * jax.nn.sigmoid(gate) * up).astype(BF16)

    def down_forward(l):
        @pl.loop(0, tokens // small)
        def _(i):
            ts = pl.ds(pl.multiple_of(i * small, small), small)
            out = dot(act[ts, :], wdn[l]).astype(BF16)
            h[l + 1, ts, :] = (h[l, ts, :].astype(F32) + out.astype(F32)).astype(BF16)

    def down_gradient(l):
        @pl.loop(0, chunks)
        def _(j):
            columns = pl.ds(pl.multiple_of(j * chunk, chunk), chunk)
            out = dot(gt[...], act[:, columns])
            term[pl.ds(pl.multiple_of(dbase + l * ff + j * chunk, chunk), chunk), :] = out.T

    def backward_tokens(l, j):
        columns = pl.ds(pl.multiple_of(j * chunk, chunk), chunk)

        @pl.loop(0, tokens // tile)
        def _(i):
            ts = pl.ds(pl.multiple_of(i * tile, tile), tile)
            gate, up = gate_up(l, ts, columns)
            by_act = dot_nt(g[ts, :], wdn[l, columns, :]).astype(BF16).astype(F32)
            sig = jax.nn.sigmoid(gate)
            silu = gate * sig
            by_up = (by_act * silu).astype(BF16)
            by_gate = (by_act * up * (sig + silu * (1.0 - sig))).astype(BF16)
            dgu[ts, :chunk] = by_gate
            dgu[ts, chunk:] = by_up
            by_a = dot_nt(by_gate, wgu[l, 0, :, columns]) + dot_nt(by_up, wgu[l, 1, :, columns])

            @pl.when(j == 0)
            def _():
                da[ts, :] = by_a

            @pl.when(j > 0)
            def _():
                da[ts, :] += by_a

    def gate_up_gradient(step, j):
        row = pl.multiple_of(lax.rem(step * chunks + j, SLOTS) * d_model, d_model)

        @pl.loop(0, 2)
        def _(i):
            columns = pl.ds(pl.multiple_of(i * chunk, chunk), chunk)
            term[pl.ds(row, d_model), columns] = dot(at[...], dgu[:, columns])

    def norm_backward(l):
        @pl.loop(0, tokens // small)
        def _(i):
            ts = pl.ds(pl.multiple_of(i * small, small), small)
            by_a = da[ts, :].astype(BF16).astype(F32)
            wide = h[l, ts, :].astype(F32)
            scale = lax.rsqrt(jnp.mean(wide * wide, -1, keepdims=True) + 1e-6)
            by_scale = jnp.sum(by_a * wide, -1, keepdims=True)
            by_wide = by_a * scale - (by_scale * scale / d_model) * (scale * scale) * wide
            g[ts, :] = (g[ts, :].astype(F32) + by_wide.astype(BF16).astype(F32)).astype(BF16)

    per = SEGMENTS + 1
    for c in loads[1:4]:
        c.wait()
    for unit in range(per):
        gather(unit, 0)
    loads[0].wait()
    normed(0)
    for k in range(1, half):
        for unit in range(per):
            gather(unit, k)
    for c in loads[4:]:
        c.wait()
    for l in range(layers):
        for s in range(SEGMENTS):
            unit = l * per + s
            gather(unit, half)
            if l + 1 < layers:
                for later in range(unit + per - s, unit + 2 * per - s):
                    gather(later, s)
            gathered(unit)
            forward(l, s)
        unit = l * per + SEGMENTS
        gather(unit, half)
        gathered(unit)
        if l + 1 < layers:
            for k in range(SEGMENTS, half):
                for later in range(unit + 1, unit + 1 + per):
                    gather(later, k)
                if k == SEGMENTS:
                    down_forward(l)
            normed(l + 1)

    for step, l in enumerate(reversed(range(layers))):
        turn()
        if step > 0:
            normed(l)
        if step > 0:
            for s in range(SEGMENTS):
                forward(l, s)
        down_gradient(l)
        start = step * per_layer
        tick(start)

        @pl.loop(0, chunks)
        def _(j):
            backward_tokens(l, j)

            @pl.when(j < subs - 1)
            def _():
                tick(start + 1 + 2 * j)

            gate_up_gradient(step, j)
            tick(start + jnp.where(j < subs - 1, 2 + 2 * j, j + subs))

        norm_backward(l)

    out_dx = pltpu.make_async_copy(g, dx_ref.at[0], load_sem.at[0])
    out_dx.start()

    @pl.loop(0, half)
    def _(i):
        tick(units + i)

    outs = [
        pltpu.make_async_copy(outg, dwg_ref, load_sem.at[1]),
        pltpu.make_async_copy(outu, dwu_ref, load_sem.at[2]),
        pltpu.make_async_copy(outd, dwd_ref, load_sem.at[3]),
    ]
    for c in outs:
        c.start()
    for direction in range(2):
        for k in range(half):
            for u in range(units - SEND, units):
                rs_copy(direction, k, u).wait_send()
    for unit in range(layers * per):
        close(unit)
    for c in (out_dx, *outs):
        c.wait()


def solution(mesh):
    n = mesh.shape["dp"]

    def step(x, dy, wg, wu, wd):
        _, tokens, d_model = x.shape
        layers, rows, ff = wg.shape
        drows = wd.shape[1]
        chunk = d_model // 2
        half = n // 2
        gather_units = layers * (SEGMENTS + 1)
        any_space = pl.BlockSpec(memory_space=pl.ANY)
        dma = pltpu.SemaphoreType.DMA
        return pl.pallas_call(
            functools.partial(kernel, n),
            out_shape=[jax.ShapeDtypeStruct(t.shape, t.dtype) for t in (x, wg, wu, wd)],
            in_specs=[any_space] * 5,
            out_specs=[any_space] * 4,
            scratch_shapes=[
                pltpu.VMEM((layers, 2, d_model, ff), BF16),
                pltpu.VMEM((layers, ff, d_model), BF16),
                pltpu.VMEM((layers, tokens, d_model), BF16),
                pltpu.VMEM((tokens, d_model), BF16),
                pltpu.VMEM((d_model, tokens), BF16),
                pltpu.VMEM((tokens, d_model), BF16),
                pltpu.VMEM((d_model, tokens), BF16),
                pltpu.VMEM((tokens, ff), BF16),
                pltpu.VMEM((tokens, 2 * chunk), BF16),
                pltpu.VMEM((tokens, d_model), F32),
                pltpu.VMEM((SLOTS * d_model + layers * ff, d_model), F32),
                pltpu.VMEM((2, half, SEND, rows, d_model), BF16),
                pltpu.VMEM((2, half, RECV, rows, d_model), BF16),
                pltpu.VMEM((layers, rows, ff), BF16),
                pltpu.VMEM((layers, rows, ff), BF16),
                pltpu.VMEM((layers, drows, d_model), BF16),
                dma((2 + 3 * layers,)),
                dma((gather_units, 2, half)),
                dma((gather_units, 2, half)),
                dma((gather_units, 2, half)),
                dma((gather_units, 2, half)),
                dma((2, half, SEND)),
                dma((2, half, RECV)),
            ],
            compiler_params=pltpu.CompilerParams(
                collective_id=0, has_side_effects=True, vmem_limit_bytes=67043328
            ),
        )(x, dy, wg, wu, wd)

    tokens_spec, weight_spec = P(("rep", "dp"), None, None), P(None, "dp", None)
    grad_spec = P("rep", "dp", None)
    return jax.shard_map(
        step,
        mesh=mesh,
        in_specs=(tokens_spec, tokens_spec, weight_spec, weight_spec, weight_spec),
        out_specs=(tokens_spec, grad_spec, grad_spec, grad_spec),
        check_vma=False,
    )
```

```python
import functools

import jax
import jax.numpy as jnp
from jax import lax
from jax.experimental import pallas as pl
from jax.experimental.pallas import tpu as pltpu
from jax.sharding import PartitionSpec as P

MESH = pl.DeviceIdType.MESH
F32, BF16 = jnp.float32, jnp.bfloat16
SEGMENTS = 2
SLOTS = 5
RECV = 8
SEND = 3
LAG = 2


def dot(a, b):
    return jnp.dot(a, b, preferred_element_type=F32)


def dot_nt(a, b):
    return lax.dot_general(a, b, (((1,), (1,)), ((), ())), preferred_element_type=F32)


def kernel(
    n, x_ref, dy_ref, wg_ref, wu_ref, wd_ref, dx_ref, dwg_ref, dwu_ref, dwd_ref, kept,
    wgu, wdn, h, g, gt, a, at, act, dgu, da, term, sbuf, rbuf, outg, outu, outd,
    load_sem, keep_sem, ag_send, ag_recv, sw_send, sw_recv, rs_send, rs_recv,
):
    layers, _, d_model, ff = wgu.shape
    tokens = h.shape[1]
    rows = d_model // n
    drows = ff // n
    chunk = d_model // 2
    chunks = ff // chunk
    subs = drows // rows
    half = n // 2
    early = 2
    per_layer = 1 + 2 * chunks + subs - early
    dbase = SLOTS * d_model
    seg = ff // SEGMENTS

    me, rep = lax.axis_index("dp"), lax.axis_index("rep")
    left, right = lax.rem(me + n - 1, n), lax.rem(me + 1, n)
    core = lax.rem(rep, 2)
    partner = rep + 1 - 2 * core
    toward = ({"dp": left}, {"dp": right})

    def at_distance(direction, k):
        return lax.rem(me + (n - k if direction == 0 else k), n)

    mine = pl.multiple_of(me * rows, rows)
    dmine = pl.multiple_of(me * drows, drows)
    loads = [pltpu.make_async_copy(x_ref.at[0], h.at[0], load_sem.at[0])]
    for l in range(layers):
        loads += [
            pltpu.make_async_copy(wg_ref.at[l], wgu.at[l, 0, pl.ds(mine, rows), :], load_sem.at[1 + 3 * l]),
            pltpu.make_async_copy(wu_ref.at[l], wgu.at[l, 1, pl.ds(mine, rows), :], load_sem.at[2 + 3 * l]),
            pltpu.make_async_copy(wd_ref.at[l], wdn.at[l, pl.ds(dmine, drows), :], load_sem.at[3 + 3 * l]),
        ]
    loads.append(pltpu.make_async_copy(dy_ref.at[0], g, load_sem.at[1 + 3 * layers]))
    for c in loads:
        c.start()

    barrier = pltpu.get_barrier_semaphore()
    for other in (*toward, {"rep": partner}):
        pl.semaphore_signal(barrier, inc=1, device_id=other, device_id_type=MESH)
    pl.semaphore_wait(barrier, 3)

    def piece(unit, origin, member, part=None):
        l, s = unit // (SEGMENTS + 1), unit % (SEGMENTS + 1)
        if s < SEGMENTS:
            size, first, width = rows // 2, s * seg, seg
            if part is not None:
                width = seg // 2
                first += part * width
            row = pl.multiple_of(origin * rows + member * size, size)
            return wgu.at[l, :, pl.ds(row, size), pl.ds(first, width)]
        size = drows // 2
        row = origin * drows + member * size
        if part is not None:
            size //= 2
            row += part * size
        return wdn.at[l, pl.ds(pl.multiple_of(row, size), size), :]

    def hop(unit, direction, k):
        origin = at_distance(1 - direction, k)
        ref = piece(unit, origin, core, direction if k == half - 1 else None)
        return pltpu.make_async_remote_copy(
            ref, ref, ag_send.at[unit, direction, k], ag_recv.at[unit, direction, k],
            device_id=toward[direction], device_id_type=MESH,
        )

    def landed(unit, direction, k):
        origin = at_distance(1 - direction, k + 1)
        ref = piece(unit, origin, core, direction if k == half - 1 else None)
        return pltpu.make_async_remote_copy(
            ref, ref, ag_send.at[unit, direction, k], ag_recv.at[unit, direction, k],
            device_id=toward[direction], device_id_type=MESH,
        )

    def swap(unit, direction, k, member):
        origin = at_distance(1 - direction, k + 1)
        ref = piece(unit, origin, member, direction if k == half - 1 else None)
        return pltpu.make_async_remote_copy(
            ref, ref, sw_send.at[unit, direction, k], sw_recv.at[unit, direction, k],
            device_id={"rep": partner}, device_id_type=MESH,
        )

    def gather(unit, k):
        for direction in range(2):
            if k > 0:
                landed(unit, direction, k - 1).wait_recv()
            if k < half:
                hop(unit, direction, k).start()
            if k > 0:
                swap(unit, direction, k - 1, core).start()

    def gathered(unit):
        for k in range(half):
            for direction in range(2):
                swap(unit, direction, k, 1 - core).wait_recv()

    def close(unit):
        for k in range(half):
            for direction in range(2):
                hop(unit, direction, k).wait_send()
                swap(unit, direction, k, core).wait_send()

    def place(u):
        step = jnp.minimum(u // per_layer, layers - 1)
        v = u - step * per_layer
        l = layers - 1 - step
        last = step == layers - 1
        soon = jnp.where(last, subs, early)
        odd = lax.rem(v, 2) == 1
        held = v - 2 * chunks - 1
        down = (v == 0) | (odd & (v < 2 * soon - 1)) | ((held >= 0) & jnp.logical_not(last))
        gate = jnp.logical_not(odd) & (v > 0) & (held < 0)
        index = jnp.where(down, jnp.where(held >= 0, held + early, (v + 1) // 2), v // 2 - 1)
        slot = lax.rem(step * chunks + jnp.maximum(index, 0), SLOTS)
        base = jnp.where(down, dbase + l * ff + index * rows, slot * d_model)
        stride = jnp.where(down, drows, rows)
        return down | gate, l, down, index, base, stride

    def rs_copy(direction, k, u):
        lo, size = (direction * (rows // 2), rows // 2) if k == 0 else (0, rows)
        return pltpu.make_async_remote_copy(
            sbuf.at[direction, k, lax.rem(u, SEND), pl.ds(lo, size), :],
            rbuf.at[direction, k, lax.rem(u, RECV), pl.ds(lo, size), :],
            rs_send.at[direction, k, lax.rem(u, SEND)],
            rs_recv.at[direction, k, lax.rem(u, RECV)],
            device_id=toward[direction],
            device_id_type=MESH,
        )

    def stage(u, k, l, down, index, base, stride):
        hrows = rows // 2

        def own(owner, lo, size):
            return term[pl.ds(pl.multiple_of(base + owner * stride + lo, hrows), size), :]

        if k == half:
            for direction in range(2):
                rs_copy(direction, half - 1, u).wait_send()
                rs_copy(direction, half - 1, u).wait_recv()
            slot = lax.rem(u, RECV)
            total = own(me, 0, rows)
            for direction in range(2):
                total += rbuf[direction, half - 1, slot].astype(F32)
            total = total.astype(BF16)

            @pl.when(down)
            def _():
                outd[l, pl.ds(pl.multiple_of(index * rows, rows), rows), :] = total

            @pl.when(jnp.logical_not(down))
            def _():
                columns = pl.ds(pl.multiple_of(index * chunk, chunk), chunk)
                outg[l, :, columns] = total[:, :chunk]
                outu[l, :, columns] = total[:, chunk:]

            return
        for direction in range(2):
            owner = at_distance(direction, half - k)
            to = sbuf.at[direction, k, lax.rem(u, SEND)]
            lo = direction * hrows
            if k == 0:
                to[pl.ds(lo, hrows), :] = own(owner, lo, hrows).astype(BF16)
            else:
                rs_copy(direction, k - 1, u).wait_send()
                rs_copy(direction, k - 1, u).wait_recv()
                came = rbuf.at[direction, k - 1, lax.rem(u, RECV)]
                if k == 1:
                    rest = hrows - lo
                    to[pl.ds(lo, hrows), :] = (own(owner, lo, hrows) + came[pl.ds(lo, hrows), :].astype(F32)).astype(BF16)
                    to[pl.ds(rest, hrows), :] = own(owner, rest, hrows).astype(BF16)
                else:
                    to[...] = (own(owner, 0, rows) + came[...].astype(F32)).astype(BF16)
            rs_copy(direction, k, u).start()

    def tick(t):
        for k in range(half + 1):
            u = t - LAG * k
            there, *rest = place(jnp.maximum(u, 0))
            pl.when((u >= 0) & there)(functools.partial(stage, u, k, *rest))

    small, tile = min(256, tokens), min(512, tokens)

    def normed(l):
        @pl.loop(0, tokens // small)
        def _(i):
            ts = pl.ds(pl.multiple_of(i * small, small), small)
            wide = h[l, ts, :].astype(F32)
            scale = lax.rsqrt(jnp.mean(wide * wide, -1, keepdims=True) + 1e-6)
            rounded = (wide * scale).astype(BF16)
            a[ts, :] = rounded
            at[:, ts] = rounded.T

    def turn():
        @pl.loop(0, tokens // small)
        def _(i):
            ts = pl.ds(pl.multiple_of(i * small, small), small)
            gt[:, ts] = g[ts, :].T

    def both(l, columns):
        return jnp.concatenate([wgu[l, 0, :, columns], wgu[l, 1, :, columns]], 1)

    def forward(l, s):
        @pl.loop(0, seg // chunk)
        def _(j):
            columns = pl.ds(pl.multiple_of(s * seg + j * chunk, chunk), chunk)
            w = both(l, columns)
            for i in range(tokens // tile):
                ts = pl.ds(i * tile, tile)
                out = dot(a[ts, :], w)
                gate, up = out[:, :chunk], out[:, chunk:]
                act[ts, columns] = (gate * jax.nn.sigmoid(gate) * up).astype(BF16)

    def down_forward(l):
        part = 2 * tile if tokens % (2 * tile) == 0 else tile

        @pl.loop(0, tokens // part)
        def _(i):
            for p in range(part // tile):
                ts = pl.ds(pl.multiple_of(i * part + p * tile, tile), tile)
                out = dot(act[ts, :], wdn[l]).astype(BF16)
                h[l + 1, ts, :] = (h[l, ts, :].astype(F32) + out.astype(F32)).astype(BF16)

    def down_gradient(l):
        @pl.loop(0, chunks // 2)
        def _(i):
            for p in range(2):
                j = 2 * i + p
                columns = pl.ds(pl.multiple_of(j * chunk, chunk), chunk)
                out = dot(gt[...], act[:, columns])
                term[pl.ds(pl.multiple_of(dbase + l * ff + j * chunk, chunk), chunk), :] = out.T

    def backward_tokens(l, j):
        columns = pl.ds(pl.multiple_of(j * chunk, chunk), chunk)
        w, w_down = both(l, columns), wdn[l, columns, :]

        def first(i):
            ts = pl.ds(i * tile, tile)
            return dot(a[ts, :], w), dot_nt(g[ts, :], w_down)

        def second(i, out, by_act):
            ts = pl.ds(i * tile, tile)
            gate, up = out[:, :chunk], out[:, chunk:]
            by_act = by_act.astype(BF16).astype(F32)
            sig = jax.nn.sigmoid(gate)
            silu = gate * sig
            by_up = (by_act * silu).astype(BF16)
            by_gate = (by_act * up * (sig + silu * (1.0 - sig))).astype(BF16)
            by_both = jnp.concatenate([by_gate, by_up], 1)
            dgu[ts, :] = by_both
            da[ts, :] += dot_nt(by_both, w)

        tiles = tokens // tile
        ready = first(0)
        for i in range(1, tiles):
            after = first(i)
            second(i - 1, *ready)
            ready = after
        second(tiles - 1, *ready)

    def gate_up_gradient(step, j):
        row = pl.multiple_of(lax.rem(step * chunks + j, SLOTS) * d_model, d_model)
        term[pl.ds(row, d_model), :] = dot(at[...], dgu[...])

    def norm_backward(l):
        @pl.loop(0, tokens // small)
        def _(i):
            ts = pl.ds(pl.multiple_of(i * small, small), small)
            by_a = da[ts, :].astype(BF16).astype(F32)
            wide = h[l, ts, :].astype(F32)
            scale = lax.rsqrt(jnp.mean(wide * wide, -1, keepdims=True) + 1e-6)
            by_scale = jnp.sum(by_a * wide, -1, keepdims=True)
            by_wide = by_a * scale - (by_scale * scale / d_model) * (scale * scale) * wide
            g[ts, :] = (g[ts, :].astype(F32) + by_wide.astype(BF16).astype(F32)).astype(BF16)

    per = SEGMENTS + 1
    for c in loads[1:4]:
        c.wait()
    for unit in range(per):
        gather(unit, 0)
    loads[0].wait()
    normed(0)
    for k in range(1, half):
        for unit in range(per):
            gather(unit, k)
    for c in loads[4:]:
        c.wait()
    keeps = []
    for l in range(layers):
        for c in keeps:
            c.wait()
        keeps = []
        for s in range(SEGMENTS):
            unit = l * per + s
            gather(unit, half)
            if l + 1 < layers:
                for later in range(unit + per - s, unit + 2 * per - s):
                    gather(later, s)
            gathered(unit)
            forward(l, s)
            if l + 1 < layers:
                columns = pl.ds(s * seg, seg)
                keeps.append(pltpu.make_async_copy(act.at[:, columns], kept.at[l, :, columns], keep_sem.at[s]))
                keeps[-1].start()
        unit = l * per + SEGMENTS
        gather(unit, half)
        gathered(unit)
        if l + 1 < layers:
            for k in range(SEGMENTS, half):
                for later in range(unit + 1, unit + 1 + per):
                    gather(later, k)
                if k == SEGMENTS:
                    down_forward(l)
            normed(l + 1)

    for step, l in enumerate(reversed(range(layers))):
        start = step * per_layer
        turn()
        if step > 0:
            normed(l)
            tick(start - 1)
            back.wait()
        da[...] = jnp.zeros_like(da)
        down_gradient(l)
        if l > 0:
            back = pltpu.make_async_copy(kept.at[l - 1], act, keep_sem.at[SEGMENTS])
            back.start()
        tick(start)

        @pl.loop(0, chunks)
        def _(j):
            backward_tokens(l, j)
            tick(start + 1 + 2 * j)
            gate_up_gradient(step, j)
            tick(start + 2 + 2 * j)

        norm_backward(l)
        if l > 0:
            for i in range(subs - early - 1):
                tick(start + 1 + 2 * chunks + i)

    out_dx = pltpu.make_async_copy(g, dx_ref.at[0], load_sem.at[0])
    out_dx.start()

    @pl.loop(0, LAG * half)
    def _(i):
        tick((layers - 1) * per_layer + 2 * chunks + 1 + i)

    outs = [
        pltpu.make_async_copy(outg, dwg_ref, load_sem.at[1]),
        pltpu.make_async_copy(outu, dwu_ref, load_sem.at[2]),
        pltpu.make_async_copy(outd, dwd_ref, load_sem.at[3]),
    ]
    for c in outs:
        c.start()
    for unit in range(layers * per):
        close(unit)
    for c in (out_dx, *outs):
        c.wait()


def solution(mesh):
    n = mesh.shape["dp"]

    def step(x, dy, wg, wu, wd):
        _, tokens, d_model = x.shape
        layers, rows, ff = wg.shape
        drows = wd.shape[1]
        chunk = d_model // 2
        half = n // 2
        gather_units = layers * (SEGMENTS + 1)
        any_space = pl.BlockSpec(memory_space=pl.ANY)
        dma = pltpu.SemaphoreType.DMA
        return pl.pallas_call(
            functools.partial(kernel, n),
            out_shape=[
                *(jax.ShapeDtypeStruct(t.shape, t.dtype) for t in (x, wg, wu, wd)),
                jax.ShapeDtypeStruct((layers - 1, tokens, ff), BF16),
            ],
            in_specs=[any_space] * 5,
            out_specs=[any_space] * 5,
            scratch_shapes=[
                pltpu.VMEM((layers, 2, d_model, ff), BF16),
                pltpu.VMEM((layers, ff, d_model), BF16),
                pltpu.VMEM((layers, tokens, d_model), BF16),
                pltpu.VMEM((tokens, d_model), BF16),
                pltpu.VMEM((d_model, tokens), BF16),
                pltpu.VMEM((tokens, d_model), BF16),
                pltpu.VMEM((d_model, tokens), BF16),
                pltpu.VMEM((tokens, ff), BF16),
                pltpu.VMEM((tokens, 2 * chunk), BF16),
                pltpu.VMEM((tokens, d_model), F32),
                pltpu.VMEM((SLOTS * d_model + layers * ff, d_model), F32),
                pltpu.VMEM((2, half, SEND, rows, d_model), BF16),
                pltpu.VMEM((2, half, RECV, rows, d_model), BF16),
                pltpu.VMEM((layers, rows, ff), BF16),
                pltpu.VMEM((layers, rows, ff), BF16),
                pltpu.VMEM((layers, drows, d_model), BF16),
                dma((2 + 3 * layers,)),
                dma((SEGMENTS + 1,)),
                dma((gather_units, 2, half)),
                dma((gather_units, 2, half)),
                dma((gather_units, 2, half)),
                dma((gather_units, 2, half)),
                dma((2, half, SEND)),
                dma((2, half, RECV)),
            ],
            compiler_params=pltpu.CompilerParams(
                collective_id=0, has_side_effects=True, vmem_limit_bytes=67043328
            ),
        )(x, dy, wg, wu, wd)[:4]

    tokens_spec, weight_spec = P(("rep", "dp"), None, None), P(None, "dp", None)
    grad_spec = P("rep", "dp", None)
    return jax.shard_map(
        step,
        mesh=mesh,
        in_specs=(tokens_spec, tokens_spec, weight_spec, weight_spec, weight_spec),
        out_specs=(tokens_spec, grad_spec, grad_spec, grad_spec),
        check_vma=False,
    )
```

```python
import functools
import math

import jax
import jax.numpy as jnp
from jax import lax
from jax.experimental import pallas as pl
from jax.experimental.pallas import tpu as pltpu
from jax.sharding import PartitionSpec as P

MESH = pl.DeviceIdType.MESH
F32, BF16 = jnp.float32, jnp.bfloat16
SEGMENTS = 2
SLOTS = 5
RECV = 8
SEND = 3
LAG = 2


def dot(a, b):
    return jnp.dot(a, b, preferred_element_type=F32)


def dot_nt(a, b):
    return lax.dot_general(a, b, (((1,), (1,)), ((), ())), preferred_element_type=F32)


def kernel(
    n, reps, x_ref, dy_ref, wg_ref, wu_ref, wd_ref, dx_ref, dwg_ref, dwu_ref, dwd_ref, kept,
    wgu, wdn, h, g, gt, a, at, act, dgu, da, term, sbuf, rbuf, outg, outu, outd,
    load_sem, keep_sem, ag_send, ag_recv, sw_send, sw_recv, y_send, y_recv, far_send, far_recv, rs_send, rs_recv,
):
    layers, _, d_model, ff = wgu.shape
    tokens = h.shape[1]
    rows = d_model // n
    drows = ff // n
    chunk = d_model // 2
    chunks = ff // chunk
    subs = drows // rows
    half = n // 2
    early = 2
    per_layer = 1 + 2 * chunks + subs - early
    dbase = SLOTS * d_model
    seg = ff // SEGMENTS

    me, rep = lax.axis_index("dp"), lax.axis_index("rep")
    left, right = lax.rem(me + n - 1, n), lax.rem(me + 1, n)
    core = lax.rem(rep, 2)
    partner = rep + 1 - 2 * core
    sides, across = [], []
    for stride in (2, 2 * math.isqrt(reps // 2)):
        sides.append(lax.rem(rep // stride, 2))
        across.append(rep + stride - 2 * stride * sides[-1])
    toward = ({"dp": left}, {"dp": right})

    def at_distance(direction, k):
        return lax.rem(me + (n - k if direction == 0 else k), n)

    mine = pl.multiple_of(me * rows, rows)
    dmine = pl.multiple_of(me * drows, drows)
    loads = [pltpu.make_async_copy(x_ref.at[0], h.at[0], load_sem.at[0])]
    for l in range(layers):
        loads += [
            pltpu.make_async_copy(wg_ref.at[l], wgu.at[l, 0, pl.ds(mine, rows), :], load_sem.at[1 + 3 * l]),
            pltpu.make_async_copy(wu_ref.at[l], wgu.at[l, 1, pl.ds(mine, rows), :], load_sem.at[2 + 3 * l]),
            pltpu.make_async_copy(wd_ref.at[l], wdn.at[l, pl.ds(dmine, drows), :], load_sem.at[3 + 3 * l]),
        ]
    loads.append(pltpu.make_async_copy(dy_ref.at[0], g, load_sem.at[1 + 3 * layers]))
    for c in loads:
        c.start()

    barrier = pltpu.get_barrier_semaphore()
    for other in (*toward, {"rep": partner}, *({"rep": r} for r in across)):
        pl.semaphore_signal(barrier, inc=1, device_id=other, device_id_type=MESH)
    pl.semaphore_wait(barrier, 5)

    def axis(unit):
        return sum(divmod(unit, SEGMENTS + 1)) % 2

    def share(unit, other_core=False, other_side=False):
        c, side = 1 - core if other_core else core, sides[axis(unit)]
        return 2 * (1 - side if other_side else side) + c

    def piece(unit, direction, k, member):
        origin = at_distance(1 - direction, k)
        l, s = unit // (SEGMENTS + 1), unit % (SEGMENTS + 1)
        parts = 4
        halved = k == half
        if s < SEGMENTS:
            size, first, width = rows // parts, s * seg, seg
            if halved:
                width = seg // 2
                first += direction * width
            row = pl.multiple_of(origin * rows + member * size, size)
            return wgu.at[l, :, pl.ds(row, size), pl.ds(first, width)]
        size = drows // parts
        row = origin * drows + member * size
        if halved:
            size //= 2
            row += direction * size
        return wdn.at[l, pl.ds(pl.multiple_of(row, size), size), :]

    def ship(sems, unit, direction, k, ref, to):
        send, recv = sems
        return pltpu.make_async_remote_copy(
            ref, ref, send.at[unit, direction, k], recv.at[unit, direction, k], device_id=to, device_id_type=MESH
        )

    def hop(unit, direction, k):
        origin = at_distance(1 - direction, k)
        ref = piece(unit, direction, k, share(unit))
        if k == half - 1:
            ref = last_half(unit, direction, origin)
        return ship((ag_send, ag_recv), unit, direction, k, ref, toward[direction])

    def last_half(unit, direction, origin):
        l, s = unit // (SEGMENTS + 1), unit % (SEGMENTS + 1)
        parts, member = 4, share(unit)
        if s < SEGMENTS:
            size, width = rows // parts, seg // 2
            row = pl.multiple_of(origin * rows + member * size, size)
            return wgu.at[l, :, pl.ds(row, size), pl.ds(s * seg + direction * width, width)]
        size = drows // parts // 2
        row = origin * drows + (2 * member + direction) * size
        return wdn.at[l, pl.ds(pl.multiple_of(row, size), size), :]

    def landed(unit, direction, k):
        ref = piece(unit, direction, k + 1, share(unit))
        return ship((ag_send, ag_recv), unit, direction, k, ref, toward[direction])

    def swap(unit, direction, k, other_core=False):
        ref = piece(unit, direction, k + 1, share(unit, other_core))
        return ship((sw_send, sw_recv), unit, direction, k, ref, {"rep": partner})

    def cross(unit, direction, k, other_side=False):
        ref = piece(unit, direction, k + 1, share(unit, False, other_side))
        return ship((y_send, y_recv), unit, direction, k, ref, {"rep": across[axis(unit)]})

    def far(unit, direction, k, other_core=False):
        ref = piece(unit, direction, k + 1, share(unit, other_core, True))
        return ship((far_send, far_recv), unit, direction, k, ref, {"rep": partner})

    def gather(unit, k):
        for direction in range(2):
            if 0 < k <= half:
                landed(unit, direction, k - 1).wait_recv()
            if k < half:
                hop(unit, direction, k).start()
            if 0 < k <= half:
                cross(unit, direction, k - 1).start()
                swap(unit, direction, k - 1).start()
        if k > 1:
            for direction in range(2):
                cross(unit, direction, k - 2, True).wait_recv()
                far(unit, direction, k - 2).start()

    def gathered(unit):
        for k in range(half):
            for direction in range(2):
                swap(unit, direction, k, True).wait_recv()
                far(unit, direction, k, True).wait_recv()

    def close(unit):
        for k in range(half):
            for direction in range(2):
                hop(unit, direction, k).wait_send()
                swap(unit, direction, k).wait_send()
                cross(unit, direction, k).wait_send()
                far(unit, direction, k).wait_send()

    def place(u):
        step = jnp.minimum(u // per_layer, layers - 1)
        v = u - step * per_layer
        l = layers - 1 - step
        last = step == layers - 1
        soon = jnp.where(last, subs, early)
        odd = lax.rem(v, 2) == 1
        held = v - 2 * chunks - 1
        down = (v == 0) | (odd & (v < 2 * soon - 1)) | ((held >= 0) & jnp.logical_not(last))
        gate = jnp.logical_not(odd) & (v > 0) & (held < 0)
        index = jnp.where(down, jnp.where(held >= 0, held + early, (v + 1) // 2), v // 2 - 1)
        slot = lax.rem(step * chunks + jnp.maximum(index, 0), SLOTS)
        base = jnp.where(down, dbase + l * ff + index * rows, slot * d_model)
        stride = jnp.where(down, drows, rows)
        return down | gate, l, down, index, base, stride

    def rs_copy(direction, k, u):
        lo, size = (direction * (rows // 2), rows // 2) if k == 0 else (0, rows)
        return pltpu.make_async_remote_copy(
            sbuf.at[direction, k, lax.rem(u, SEND), pl.ds(lo, size), :],
            rbuf.at[direction, k, lax.rem(u, RECV), pl.ds(lo, size), :],
            rs_send.at[direction, k, lax.rem(u, SEND)],
            rs_recv.at[direction, k, lax.rem(u, RECV)],
            device_id=toward[direction],
            device_id_type=MESH,
        )

    def stage(u, k, l, down, index, base, stride):
        hrows = rows // 2

        def own(owner, lo, size):
            return term[pl.ds(pl.multiple_of(base + owner * stride + lo, hrows), size), :]

        if k == half:
            for direction in range(2):
                rs_copy(direction, half - 1, u).wait_send()
                rs_copy(direction, half - 1, u).wait_recv()
            slot = lax.rem(u, RECV)
            total = own(me, 0, rows)
            for direction in range(2):
                total += rbuf[direction, half - 1, slot].astype(F32)
            total = total.astype(BF16)

            @pl.when(down)
            def _():
                outd[l, pl.ds(pl.multiple_of(index * rows, rows), rows), :] = total

            @pl.when(jnp.logical_not(down))
            def _():
                columns = pl.ds(pl.multiple_of(index * chunk, chunk), chunk)
                outg[l, :, columns] = total[:, :chunk]
                outu[l, :, columns] = total[:, chunk:]

            return
        for direction in range(2):
            owner = at_distance(direction, half - k)
            to = sbuf.at[direction, k, lax.rem(u, SEND)]
            lo = direction * hrows
            if k == 0:
                to[pl.ds(lo, hrows), :] = own(owner, lo, hrows).astype(BF16)
            else:
                rs_copy(direction, k - 1, u).wait_send()
                rs_copy(direction, k - 1, u).wait_recv()
                came = rbuf.at[direction, k - 1, lax.rem(u, RECV)]
                if k == 1:
                    rest = hrows - lo
                    to[pl.ds(lo, hrows), :] = (own(owner, lo, hrows) + came[pl.ds(lo, hrows), :].astype(F32)).astype(BF16)
                    to[pl.ds(rest, hrows), :] = own(owner, rest, hrows).astype(BF16)
                else:
                    to[...] = (own(owner, 0, rows) + came[...].astype(F32)).astype(BF16)
            rs_copy(direction, k, u).start()

    def tick(t):
        for k in range(half + 1):
            u = t - LAG * k
            there, *rest = place(jnp.maximum(u, 0))
            pl.when((u >= 0) & there)(functools.partial(stage, u, k, *rest))

    small, tile = min(256, tokens), min(512, tokens)

    def normed(l):
        @pl.loop(0, tokens // small)
        def _(i):
            ts = pl.ds(pl.multiple_of(i * small, small), small)
            wide = h[l, ts, :].astype(F32)
            scale = lax.rsqrt(jnp.mean(wide * wide, -1, keepdims=True) + 1e-6)
            rounded = (wide * scale).astype(BF16)
            a[ts, :] = rounded
            at[:, ts] = rounded.T

    def turn():
        @pl.loop(0, tokens // small)
        def _(i):
            ts = pl.ds(pl.multiple_of(i * small, small), small)
            gt[:, ts] = g[ts, :].T

    def both(l, columns):
        return jnp.concatenate([wgu[l, 0, :, columns], wgu[l, 1, :, columns]], 1)

    def forward(l, s, *between):
        @pl.loop(0, seg // chunk)
        def _(j):
            columns = pl.ds(pl.multiple_of(s * seg + j * chunk, chunk), chunk)
            w = both(l, columns)
            for i in range(tokens // tile):
                ts = pl.ds(i * tile, tile)
                out = dot(a[ts, :], w)
                gate, up = out[:, :chunk], out[:, chunk:]
                act[ts, columns] = (gate * jax.nn.sigmoid(gate) * up).astype(BF16)
            for number, steps in enumerate(between):
                if steps:
                    pl.when(j == number)(functools.partial(gathers, *steps))

    def down_forward(l):
        part = 2 * tile if tokens % (2 * tile) == 0 else tile

        @pl.loop(0, tokens // part)
        def _(i):
            for p in range(part // tile):
                ts = pl.ds(pl.multiple_of(i * part + p * tile, tile), tile)
                out = dot(act[ts, :], wdn[l]).astype(BF16)
                h[l + 1, ts, :] = (h[l, ts, :].astype(F32) + out.astype(F32)).astype(BF16)

    def down_gradient(l):
        @pl.loop(0, chunks // 2)
        def _(i):
            for p in range(2):
                j = 2 * i + p
                columns = pl.ds(pl.multiple_of(j * chunk, chunk), chunk)
                out = dot(gt[...], act[:, columns])
                term[pl.ds(pl.multiple_of(dbase + l * ff + j * chunk, chunk), chunk), :] = out.T

    def backward_tokens(l, j):
        columns = pl.ds(pl.multiple_of(j * chunk, chunk), chunk)
        w, w_down = both(l, columns), wdn[l, columns, :]

        def first(i):
            ts = pl.ds(i * tile, tile)
            return dot(a[ts, :], w), dot_nt(g[ts, :], w_down)

        def second(i, out, by_act):
            ts = pl.ds(i * tile, tile)
            gate, up = out[:, :chunk], out[:, chunk:]
            by_act = by_act.astype(BF16).astype(F32)
            sig = jax.nn.sigmoid(gate)
            silu = gate * sig
            by_up = (by_act * silu).astype(BF16)
            by_gate = (by_act * up * (sig + silu * (1.0 - sig))).astype(BF16)
            by_both = jnp.concatenate([by_gate, by_up], 1)
            dgu[ts, :] = by_both
            da[ts, :] += dot_nt(by_both, w)

        tiles = tokens // tile
        ready = first(0)
        for i in range(1, tiles):
            after = first(i)
            second(i - 1, *ready)
            ready = after
        second(tiles - 1, *ready)

    def gate_up_gradient(step, j):
        row = pl.multiple_of(lax.rem(step * chunks + j, SLOTS) * d_model, d_model)
        term[pl.ds(row, d_model), :] = dot(at[...], dgu[...])

    def norm_backward(l):
        @pl.loop(0, tokens // small)
        def _(i):
            ts = pl.ds(pl.multiple_of(i * small, small), small)
            by_a = da[ts, :].astype(BF16).astype(F32)
            wide = h[l, ts, :].astype(F32)
            scale = lax.rsqrt(jnp.mean(wide * wide, -1, keepdims=True) + 1e-6)
            by_scale = jnp.sum(by_a * wide, -1, keepdims=True)
            by_wide = by_a * scale - (by_scale * scale / d_model) * (scale * scale) * wide
            g[ts, :] = (g[ts, :].astype(F32) + by_wide.astype(BF16).astype(F32)).astype(BF16)

    per = SEGMENTS + 1

    def gathers(*pairs):
        for unit, k in pairs:
            gather(unit, k)

    for c in loads[1:4]:
        c.wait()
    gathers((0, 0), (1, 0))
    loads[0].wait()
    normed(0)
    gathers((0, 1), (1, 1))
    gathers((0, 2), (1, 2), (2, 0))
    gathers((0, 3), (1, 3), (2, 1))
    for c in loads[4:]:
        c.wait()
    keeps = []
    for l in range(layers):
        first, second, down = (l * per + i for i in range(per))
        last = l + 1 == layers
        ahead = () if last else ((first + per, 0), (second + per, 0))
        gathers(*ahead, (first, 4), (second, 4), (down, 2))
        if l > 0:
            normed(l)
        gather(first, 5)
        for c in keeps:
            c.wait()
        keeps = []

        def keep(s):
            if not last:
                columns = pl.ds(s * seg, seg)
                keeps.append(pltpu.make_async_copy(act.at[:, columns], kept.at[l, :, columns], keep_sem.at[s]))
                keeps[-1].start()

        def ahead(*steps):
            return () if last else tuple((i + per, k) for i, k in steps)

        gathered(first)
        forward(
            l, 0, ((second, 5), (down, 3)), ahead((first, 1), (second, 1)), ((down, 4),), ahead((down, 0))
        )
        keep(0)
        gathered(second)
        forward(
            l, 1, ahead((first, 2), (second, 2)), ((down, 5),), ahead((down, 1)), ahead((first, 3), (second, 3))
        )
        keep(1)
        gathered(down)
        if not last:
            down_forward(l)

    for step, l in enumerate(reversed(range(layers))):
        start = step * per_layer
        turn()
        if step > 0:
            normed(l)
            tick(start - 1)
            back.wait()
        da[...] = jnp.zeros_like(da)
        down_gradient(l)
        if l > 0:
            back = pltpu.make_async_copy(kept.at[l - 1], act, keep_sem.at[SEGMENTS])
            back.start()
        tick(start)

        @pl.loop(0, chunks)
        def _(j):
            backward_tokens(l, j)
            tick(start + 1 + 2 * j)
            gate_up_gradient(step, j)
            tick(start + 2 + 2 * j)

        norm_backward(l)
        if l > 0:
            for i in range(subs - early - 1):
                tick(start + 1 + 2 * chunks + i)

    out_dx = pltpu.make_async_copy(g, dx_ref.at[0], load_sem.at[0])
    out_dx.start()

    @pl.loop(0, LAG * half)
    def _(i):
        tick((layers - 1) * per_layer + 2 * chunks + 1 + i)

    outs = [
        pltpu.make_async_copy(outg, dwg_ref, load_sem.at[1]),
        pltpu.make_async_copy(outu, dwu_ref, load_sem.at[2]),
        pltpu.make_async_copy(outd, dwd_ref, load_sem.at[3]),
    ]
    for c in outs:
        c.start()
    for unit in range(layers * per):
        close(unit)
    for c in (out_dx, *outs):
        c.wait()


def solution(mesh):
    n = mesh.shape["dp"]

    def step(x, dy, wg, wu, wd):
        _, tokens, d_model = x.shape
        layers, rows, ff = wg.shape
        drows = wd.shape[1]
        chunk = d_model // 2
        half = n // 2
        gather_units = layers * (SEGMENTS + 1)
        any_space = pl.BlockSpec(memory_space=pl.ANY)
        dma = pltpu.SemaphoreType.DMA
        return pl.pallas_call(
            functools.partial(kernel, n, mesh.shape["rep"]),
            out_shape=[
                *(jax.ShapeDtypeStruct(t.shape, t.dtype) for t in (x, wg, wu, wd)),
                jax.ShapeDtypeStruct((layers - 1, tokens, ff), BF16),
            ],
            in_specs=[any_space] * 5,
            out_specs=[any_space] * 5,
            scratch_shapes=[
                pltpu.VMEM((layers, 2, d_model, ff), BF16),
                pltpu.VMEM((layers, ff, d_model), BF16),
                pltpu.VMEM((layers, tokens, d_model), BF16),
                pltpu.VMEM((tokens, d_model), BF16),
                pltpu.VMEM((d_model, tokens), BF16),
                pltpu.VMEM((tokens, d_model), BF16),
                pltpu.VMEM((d_model, tokens), BF16),
                pltpu.VMEM((tokens, ff), BF16),
                pltpu.VMEM((tokens, 2 * chunk), BF16),
                pltpu.VMEM((tokens, d_model), F32),
                pltpu.VMEM((SLOTS * d_model + layers * ff, d_model), F32),
                pltpu.VMEM((2, half, SEND, rows, d_model), BF16),
                pltpu.VMEM((2, half, RECV, rows, d_model), BF16),
                pltpu.VMEM((layers, rows, ff), BF16),
                pltpu.VMEM((layers, rows, ff), BF16),
                pltpu.VMEM((layers, drows, d_model), BF16),
                dma((2 + 3 * layers,)),
                dma((SEGMENTS + 1,)),
                dma((gather_units, 2, half)),
                dma((gather_units, 2, half)),
                dma((gather_units, 2, half)),
                dma((gather_units, 2, half)),
                dma((gather_units, 2, half)),
                dma((gather_units, 2, half)),
                dma((gather_units, 2, half)),
                dma((gather_units, 2, half)),
                dma((2, half, SEND)),
                dma((2, half, RECV)),
            ],
            compiler_params=pltpu.CompilerParams(
                collective_id=0, has_side_effects=True, vmem_limit_bytes=67043328
            ),
        )(x, dy, wg, wu, wd)[:4]

    tokens_spec, weight_spec = P(("rep", "dp"), None, None), P(None, "dp", None)
    grad_spec = P("rep", "dp", None)
    return jax.shard_map(
        step,
        mesh=mesh,
        in_specs=(tokens_spec, tokens_spec, weight_spec, weight_spec, weight_spec),
        out_specs=(tokens_spec, grad_spec, grad_spec, grad_spec),
        check_vma=False,
    )
```

```python
import functools
import math

import jax
import jax.numpy as jnp
from jax import lax
from jax.experimental import pallas as pl
from jax.experimental.pallas import tpu as pltpu
from jax.sharding import PartitionSpec as P

MESH = pl.DeviceIdType.MESH
F32, BF16 = jnp.float32, jnp.bfloat16
SEGMENTS = 2
SLOTS = 7
RECV = 8
SEND = 4
LAG = 3


def dot(a, b):
    return jnp.dot(a, b, preferred_element_type=F32)


def dot_nt(a, b):
    return lax.dot_general(a, b, (((1,), (1,)), ((), ())), preferred_element_type=F32)


def kernel(
    n, reps, x_ref, dy_ref, wg_ref, wu_ref, wd_ref, dx_ref, dwg_ref, dwu_ref, dwd_ref, kept,
    wgu, wdn, h, g, gt, a, at, act, dgu, da, term, sbuf, rbuf, outg, outu, outd,
    load_sem, keep_sem, ag_send, ag_recv, sw_send, sw_recv, y_send, y_recv, far_send, far_recv, rs_send, rs_recv,
):
    layers, _, d_model, ff = wgu.shape
    tokens = h.shape[1]
    rows = d_model // n
    drows = ff // n
    chunk = d_model // 2
    chunks = ff // chunk
    subs = drows // rows
    half = n // 2
    lead = subs - 1
    changing = 3
    per_layer = lead + 2 * chunks + changing
    dbase = SLOTS * d_model
    seg = ff // SEGMENTS

    me, rep = lax.axis_index("dp"), lax.axis_index("rep")
    left, right = lax.rem(me + n - 1, n), lax.rem(me + 1, n)
    core = lax.rem(rep, 2)
    partner = rep + 1 - 2 * core
    sides, across = [], []
    for stride in (2, 2 * math.isqrt(reps // 2)):
        sides.append(lax.rem(rep // stride, 2))
        across.append(rep + stride - 2 * stride * sides[-1])
    toward = ({"dp": left}, {"dp": right})

    def at_distance(direction, k):
        return lax.rem(me + (n - k if direction == 0 else k), n)

    mine = pl.multiple_of(me * rows, rows)
    dmine = pl.multiple_of(me * drows, drows)
    loads = [pltpu.make_async_copy(x_ref.at[0], h.at[0], load_sem.at[0])]
    for l in range(layers):
        loads += [
            pltpu.make_async_copy(wg_ref.at[l], wgu.at[l, 0, pl.ds(mine, rows), :], load_sem.at[1 + 3 * l]),
            pltpu.make_async_copy(wu_ref.at[l], wgu.at[l, 1, pl.ds(mine, rows), :], load_sem.at[2 + 3 * l]),
            pltpu.make_async_copy(wd_ref.at[l], wdn.at[l, pl.ds(dmine, drows), :], load_sem.at[3 + 3 * l]),
        ]
    loads.append(pltpu.make_async_copy(dy_ref.at[0], g, load_sem.at[1 + 3 * layers]))
    for c in loads:
        c.start()

    barrier = pltpu.get_barrier_semaphore()
    for other in (*toward, {"rep": partner}, *({"rep": r} for r in across)):
        pl.semaphore_signal(barrier, inc=1, device_id=other, device_id_type=MESH)
    pl.semaphore_wait(barrier, 5)

    def axis(unit):
        return sum(divmod(unit, SEGMENTS + 1)) % 2

    def share(unit, other_core=False, other_side=False):
        c, side = 1 - core if other_core else core, sides[axis(unit)]
        return 2 * (1 - side if other_side else side) + c

    def piece(unit, direction, k, member):
        origin = at_distance(1 - direction, k)
        l, s = unit // (SEGMENTS + 1), unit % (SEGMENTS + 1)
        parts = 4
        halved = k == half
        if s < SEGMENTS:
            size, first, width = rows // parts, s * seg, seg
            if halved:
                width = seg // 2
                first += direction * width
            row = pl.multiple_of(origin * rows + member * size, size)
            return wgu.at[l, :, pl.ds(row, size), pl.ds(first, width)]
        size = drows // parts
        row = origin * drows + member * size
        if halved:
            size //= 2
            row += direction * size
        return wdn.at[l, pl.ds(pl.multiple_of(row, size), size), :]

    def ship(sems, unit, direction, k, ref, to):
        send, recv = sems
        return pltpu.make_async_remote_copy(
            ref, ref, send.at[unit, direction, k], recv.at[unit, direction, k], device_id=to, device_id_type=MESH
        )

    def hop(unit, direction, k):
        origin = at_distance(1 - direction, k)
        ref = piece(unit, direction, k, share(unit))
        if k == half - 1:
            ref = last_half(unit, direction, origin)
        return ship((ag_send, ag_recv), unit, direction, k, ref, toward[direction])

    def last_half(unit, direction, origin):
        l, s = unit // (SEGMENTS + 1), unit % (SEGMENTS + 1)
        parts, member = 4, share(unit)
        if s < SEGMENTS:
            size, width = rows // parts, seg // 2
            row = pl.multiple_of(origin * rows + member * size, size)
            return wgu.at[l, :, pl.ds(row, size), pl.ds(s * seg + direction * width, width)]
        size = drows // parts // 2
        row = origin * drows + (2 * member + direction) * size
        return wdn.at[l, pl.ds(pl.multiple_of(row, size), size), :]

    def landed(unit, direction, k):
        ref = piece(unit, direction, k + 1, share(unit))
        return ship((ag_send, ag_recv), unit, direction, k, ref, toward[direction])

    def swap(unit, direction, k, other_core=False):
        ref = piece(unit, direction, k + 1, share(unit, other_core))
        return ship((sw_send, sw_recv), unit, direction, k, ref, {"rep": partner})

    def cross(unit, direction, k, other_side=False):
        ref = piece(unit, direction, k + 1, share(unit, False, other_side))
        return ship((y_send, y_recv), unit, direction, k, ref, {"rep": across[axis(unit)]})

    def far(unit, direction, k, other_core=False):
        ref = piece(unit, direction, k + 1, share(unit, other_core, True))
        return ship((far_send, far_recv), unit, direction, k, ref, {"rep": partner})

    def gather(unit, k):
        for direction in range(2):
            if 0 < k <= half:
                landed(unit, direction, k - 1).wait_recv()
            if k < half:
                hop(unit, direction, k).start()
            if 0 < k <= half:
                cross(unit, direction, k - 1).start()
                swap(unit, direction, k - 1).start()
        if k > 1:
            for direction in range(2):
                cross(unit, direction, k - 2, True).wait_recv()
                far(unit, direction, k - 2).start()

    def gathered(unit):
        for k in range(half):
            for direction in range(2):
                swap(unit, direction, k, True).wait_recv()
                far(unit, direction, k, True).wait_recv()

    def close(unit):
        for k in range(half):
            for direction in range(2):
                hop(unit, direction, k).wait_send()
                swap(unit, direction, k).wait_send()
                cross(unit, direction, k).wait_send()
                far(unit, direction, k).wait_send()

    def place(u):
        step = jnp.minimum(u // per_layer, layers - 1)
        l = layers - 1 - step
        last = step == layers - 1
        first = jnp.where(last, 1, lead)
        v = u - step * per_layer
        r = v - first
        held = r - 2 * chunks
        even = lax.rem(jnp.maximum(r, 0), 2) == 0
        beside = last & even & (r >= 0) & (r < 2 * (subs - 1))
        down = (r < 0) | beside | ((held == 0) & jnp.logical_not(last))
        gate = jnp.logical_not(even) & (r > 0) & (held < 0)
        index = jnp.where(r < 0, v, jnp.where(held == 0, lead, jnp.where(beside, 1 + r // 2, r // 2)))
        slot = lax.rem(step * chunks + jnp.maximum(index, 0), SLOTS)
        base = jnp.where(down, dbase + l * ff + index * rows, slot * d_model)
        stride = jnp.where(down, drows, rows)
        return down | gate, l, down, index, base, stride

    def rs_copy(direction, k, u):
        lo, size = (direction * (rows // 2), rows // 2) if k == 0 else (0, rows)
        return pltpu.make_async_remote_copy(
            sbuf.at[direction, k, lax.rem(u, SEND), pl.ds(lo, size), :],
            rbuf.at[direction, k, lax.rem(u, RECV), pl.ds(lo, size), :],
            rs_send.at[direction, k, lax.rem(u, SEND)],
            rs_recv.at[direction, k, lax.rem(u, RECV)],
            device_id=toward[direction],
            device_id_type=MESH,
        )

    def stage(u, k, l, down, index, base, stride):
        hrows = rows // 2

        def own(owner, lo, size):
            return term[pl.ds(pl.multiple_of(base + owner * stride + lo, hrows), size), :]

        if k == half:
            for direction in range(2):
                rs_copy(direction, half - 1, u).wait_send()
                rs_copy(direction, half - 1, u).wait_recv()
            slot = lax.rem(u, RECV)
            total = own(me, 0, rows)
            for direction in range(2):
                total += rbuf[direction, half - 1, slot].astype(F32)
            total = total.astype(BF16)

            @pl.when(down)
            def _():
                outd[l, pl.ds(pl.multiple_of(index * rows, rows), rows), :] = total

            @pl.when(jnp.logical_not(down))
            def _():
                columns = pl.ds(pl.multiple_of(index * chunk, chunk), chunk)
                outg[l, :, columns] = total[:, :chunk]
                outu[l, :, columns] = total[:, chunk:]

            return
        for direction in range(2):
            owner = at_distance(direction, half - k)
            to = sbuf.at[direction, k, lax.rem(u, SEND)]
            lo = direction * hrows
            if k == 0:
                to[pl.ds(lo, hrows), :] = own(owner, lo, hrows).astype(BF16)
            else:
                rs_copy(direction, k - 1, u).wait_send()
                rs_copy(direction, k - 1, u).wait_recv()
                came = rbuf.at[direction, k - 1, lax.rem(u, RECV)]
                if k == 1:
                    rest = hrows - lo
                    to[pl.ds(lo, hrows), :] = (own(owner, lo, hrows) + came[pl.ds(lo, hrows), :].astype(F32)).astype(BF16)
                    to[pl.ds(rest, hrows), :] = own(owner, rest, hrows).astype(BF16)
                else:
                    to[...] = (own(owner, 0, rows) + came[...].astype(F32)).astype(BF16)
            rs_copy(direction, k, u).start()

    def tick(t):
        for k in range(half + 1):
            u = t - LAG * k
            there, *rest = place(jnp.maximum(u, 0))
            pl.when((u >= 0) & there)(functools.partial(stage, u, k, *rest))

    small, tile = min(256, tokens), min(512, tokens)

    def normed(l):
        @pl.loop(0, tokens // small)
        def _(i):
            ts = pl.ds(pl.multiple_of(i * small, small), small)
            wide = h[l, ts, :].astype(F32)
            scale = lax.rsqrt(jnp.mean(wide * wide, -1, keepdims=True) + 1e-6)
            rounded = (wide * scale).astype(BF16)
            a[ts, :] = rounded
            at[:, ts] = rounded.T

    def turn():
        @pl.loop(0, tokens // small)
        def _(i):
            ts = pl.ds(pl.multiple_of(i * small, small), small)
            gt[:, ts] = g[ts, :].T

    def both(l, columns):
        return jnp.concatenate([wgu[l, 0, :, columns], wgu[l, 1, :, columns]], 1)

    def forward(l, s, *between):
        @pl.loop(0, seg // chunk)
        def _(j):
            columns = pl.ds(pl.multiple_of(s * seg + j * chunk, chunk), chunk)
            w = both(l, columns)
            for i in range(tokens // tile):
                ts = pl.ds(i * tile, tile)
                out = dot(a[ts, :], w)
                gate, up = out[:, :chunk], out[:, chunk:]
                act[ts, columns] = (gate * jax.nn.sigmoid(gate) * up).astype(BF16)
            for number, steps in enumerate(between):
                if steps:
                    pl.when(j == number)(functools.partial(gathers, *steps))

    def down_forward(l):
        part = 2 * tile if tokens % (2 * tile) == 0 else tile

        @pl.loop(0, tokens // part)
        def _(i):
            for p in range(part // tile):
                ts = pl.ds(pl.multiple_of(i * part + p * tile, tile), tile)
                out = dot(act[ts, :], wdn[l]).astype(BF16)
                h[l + 1, ts, :] = (h[l, ts, :].astype(F32) + out.astype(F32)).astype(BF16)

    def down_gradient(l, start):
        @pl.loop(0, chunks // 2)
        def _(i):
            for p in range(2):
                j = 2 * i + p
                columns = pl.ds(pl.multiple_of(j * chunk, chunk), chunk)
                out = dot(gt[...], act[:, columns])
                term[pl.ds(pl.multiple_of(dbase + l * ff + j * chunk, chunk), chunk), :] = out.T
            if start > 0:
                pl.when(i == 1)(functools.partial(tick, start - 1))

    def backward_tokens(l, j):
        columns = pl.ds(pl.multiple_of(j * chunk, chunk), chunk)
        w, w_down = both(l, columns), wdn[l, columns, :]

        def first(i):
            ts = pl.ds(i * tile, tile)
            return dot(a[ts, :], w), dot_nt(g[ts, :], w_down)

        def second(i, out, by_act):
            ts = pl.ds(i * tile, tile)
            gate, up = out[:, :chunk], out[:, chunk:]
            by_act = by_act.astype(BF16).astype(F32)
            sig = jax.nn.sigmoid(gate)
            silu = gate * sig
            by_up = (by_act * silu).astype(BF16)
            by_gate = (by_act * up * (sig + silu * (1.0 - sig))).astype(BF16)
            by_both = jnp.concatenate([by_gate, by_up], 1)
            dgu[ts, :] = by_both
            da[ts, :] += dot_nt(by_both, w)

        tiles = tokens // tile
        ready = first(0)
        for i in range(1, tiles):
            after = first(i)
            second(i - 1, *ready)
            ready = after
        second(tiles - 1, *ready)

    def gate_up_gradient(step, j):
        row = pl.multiple_of(lax.rem(step * chunks + j, SLOTS) * d_model, d_model)
        term[pl.ds(row, d_model), :] = dot(at[...], dgu[...])

    def norm_backward(l):
        @pl.loop(0, tokens // small)
        def _(i):
            ts = pl.ds(pl.multiple_of(i * small, small), small)
            by_a = da[ts, :].astype(BF16).astype(F32)
            wide = h[l, ts, :].astype(F32)
            scale = lax.rsqrt(jnp.mean(wide * wide, -1, keepdims=True) + 1e-6)
            by_scale = jnp.sum(by_a * wide, -1, keepdims=True)
            by_wide = by_a * scale - (by_scale * scale / d_model) * (scale * scale) * wide
            g[ts, :] = (g[ts, :].astype(F32) + by_wide.astype(BF16).astype(F32)).astype(BF16)

    per = SEGMENTS + 1

    def gathers(*pairs):
        for unit, k in pairs:
            gather(unit, k)

    for c in loads[1:4]:
        c.wait()
    gathers((0, 0), (1, 0))
    loads[0].wait()
    normed(0)
    for c in loads[4:-1]:
        c.wait()
    gathers((2, 0), (3, 0), (0, 1), (1, 1), (2, 1), (3, 1), (0, 2), (1, 2), (2, 2), (3, 2), (0, 3), (4, 0), (1, 3))
    loads[-1].wait()
    turn()
    gathers((2, 3), (5, 0), (3, 3), (0, 4), (4, 1), (1, 4), (2, 4), (5, 1), (0, 5), (3, 4))
    between = (
        (((1, 5), (4, 2)), (), ((2, 5), (5, 2)), ((3, 5),)),
        ((), ((4, 3),), (), ((5, 3),)),
        (((4, 4),), ((5, 4),), (), ((4, 5), (5, 5))),
        (),
    )
    keeps = []
    for l in range(layers):
        last = l + 1 == layers
        if l > 0:
            normed(l)
        for c in keeps:
            c.wait()
        keeps = []
        for i in range(SEGMENTS):
            gathered(l * per + i)
            forward(l, i, *between[l * SEGMENTS + i])
            if not last:
                columns = pl.ds(i * seg, seg)
                keeps.append(pltpu.make_async_copy(act.at[:, columns], kept.at[l, :, columns], keep_sem.at[i]))
                keeps[-1].start()
        gathered(l * per + SEGMENTS)
        if not last:
            down_forward(l)

    for step, l in enumerate(reversed(range(layers))):
        start = step * per_layer
        count = lead if l > 0 else 1
        da[...] = jnp.zeros_like(da)
        if step > 0:
            turn()
            normed(l)
            tick(start - 2)
            back.wait()
        down_gradient(l, start)
        if l > 0:
            back = pltpu.make_async_copy(kept.at[l - 1], act, keep_sem.at[SEGMENTS])
            back.start()

        @pl.loop(0, count)
        def _(i):
            tick(start + i)

        @pl.loop(0, chunks)
        def _(j):
            backward_tokens(l, j)
            tick(start + count + 2 * j)
            gate_up_gradient(step, j)
            tick(start + count + 1 + 2 * j)

        norm_backward(l)
        if l > 0:
            tick(start + count + 2 * chunks)

    out_dx = pltpu.make_async_copy(g, dx_ref.at[0], load_sem.at[0])
    out_dx.start()

    @pl.loop(0, LAG * half)
    def _(i):
        tick((layers - 1) * per_layer + 1 + 2 * chunks + i)

    outs = [
        pltpu.make_async_copy(outg, dwg_ref, load_sem.at[1]),
        pltpu.make_async_copy(outu, dwu_ref, load_sem.at[2]),
        pltpu.make_async_copy(outd, dwd_ref, load_sem.at[3]),
    ]
    for c in outs:
        c.start()
    for unit in range(layers * per):
        close(unit)
    for c in (out_dx, *outs):
        c.wait()


def solution(mesh):
    n = mesh.shape["dp"]

    def step(x, dy, wg, wu, wd):
        _, tokens, d_model = x.shape
        layers, rows, ff = wg.shape
        drows = wd.shape[1]
        chunk = d_model // 2
        half = n // 2
        gather_units = layers * (SEGMENTS + 1)
        any_space = pl.BlockSpec(memory_space=pl.ANY)
        dma = pltpu.SemaphoreType.DMA
        return pl.pallas_call(
            functools.partial(kernel, n, mesh.shape["rep"]),
            out_shape=[
                *(jax.ShapeDtypeStruct(t.shape, t.dtype) for t in (x, wg, wu, wd)),
                jax.ShapeDtypeStruct((layers - 1, tokens, ff), BF16),
            ],
            in_specs=[any_space] * 5,
            out_specs=[any_space] * 5,
            scratch_shapes=[
                pltpu.VMEM((layers, 2, d_model, ff), BF16),
                pltpu.VMEM((layers, ff, d_model), BF16),
                pltpu.VMEM((layers, tokens, d_model), BF16),
                pltpu.VMEM((tokens, d_model), BF16),
                pltpu.VMEM((d_model, tokens), BF16),
                pltpu.VMEM((tokens, d_model), BF16),
                pltpu.VMEM((d_model, tokens), BF16),
                pltpu.VMEM((tokens, ff), BF16),
                pltpu.VMEM((tokens, 2 * chunk), BF16),
                pltpu.VMEM((tokens, d_model), F32),
                pltpu.VMEM((SLOTS * d_model + layers * ff, d_model), F32),
                pltpu.VMEM((2, half, SEND, rows, d_model), BF16),
                pltpu.VMEM((2, half, RECV, rows, d_model), BF16),
                pltpu.VMEM((layers, rows, ff), BF16),
                pltpu.VMEM((layers, rows, ff), BF16),
                pltpu.VMEM((layers, drows, d_model), BF16),
                dma((2 + 3 * layers,)),
                dma((SEGMENTS + 1,)),
                dma((gather_units, 2, half)),
                dma((gather_units, 2, half)),
                dma((gather_units, 2, half)),
                dma((gather_units, 2, half)),
                dma((gather_units, 2, half)),
                dma((gather_units, 2, half)),
                dma((gather_units, 2, half)),
                dma((gather_units, 2, half)),
                dma((2, half, SEND)),
                dma((2, half, RECV)),
            ],
            compiler_params=pltpu.CompilerParams(
                collective_id=0, has_side_effects=True, vmem_limit_bytes=67043328
            ),
        )(x, dy, wg, wu, wd)[:4]

    tokens_spec, weight_spec = P(("rep", "dp"), None, None), P(None, "dp", None)
    grad_spec = P("rep", "dp", None)
    return jax.shard_map(
        step,
        mesh=mesh,
        in_specs=(tokens_spec, tokens_spec, weight_spec, weight_spec, weight_spec),
        out_specs=(tokens_spec, grad_spec, grad_spec, grad_spec),
        check_vma=False,
    )
```

```python
import functools
import math

import jax
import jax.numpy as jnp
from jax import lax
from jax.experimental import pallas as pl
from jax.experimental.pallas import tpu as pltpu
from jax.sharding import PartitionSpec as P

MESH = pl.DeviceIdType.MESH
F32, BF16 = jnp.float32, jnp.bfloat16
SEGMENTS = 2
SLOTS = 7
RECV = 8
SEND = 4
LAG = 3


def dot(a, b):
    return jnp.dot(a, b, preferred_element_type=F32)


def dot_nt(a, b):
    return lax.dot_general(a, b, (((1,), (1,)), ((), ())), preferred_element_type=F32)


def kernel(
    n, reps, x_ref, dy_ref, wg_ref, wu_ref, wd_ref, dx_ref, dwg_ref, dwu_ref, dwd_ref, kept,
    wgu, wdn, h, g, gt, a, at, act, dgu, da, term, sbuf, rbuf, outg, outu, outd,
    load_sem, keep_sem, ag_send, ag_recv, sw_send, sw_recv, y_send, y_recv, far_send, far_recv, rs_send, rs_recv,
):
    layers, _, d_model, ff = wgu.shape
    tokens = h.shape[1]
    rows = d_model // n
    drows = ff // n
    chunk = d_model // 2
    chunks = ff // chunk
    subs = drows // rows
    half = n // 2
    lead = subs - 1
    changing = 3
    per_layer = lead + 2 * chunks + changing
    dbase = SLOTS * d_model
    seg = ff // SEGMENTS

    me, rep = lax.axis_index("dp"), lax.axis_index("rep")
    left, right = lax.rem(me + n - 1, n), lax.rem(me + 1, n)
    core = lax.rem(rep, 2)
    partner = rep + 1 - 2 * core
    sides, across = [], []
    for stride in (2, 2 * math.isqrt(reps // 2)):
        sides.append(lax.rem(rep // stride, 2))
        across.append(rep + stride - 2 * stride * sides[-1])
    toward = ({"dp": left}, {"dp": right})

    def at_distance(direction, k):
        return lax.rem(me + (n - k if direction == 0 else k), n)

    mine = pl.multiple_of(me * rows, rows)
    dmine = pl.multiple_of(me * drows, drows)
    loads = [pltpu.make_async_copy(x_ref.at[0], h.at[0], load_sem.at[0])]
    for l in range(layers):
        loads += [
            pltpu.make_async_copy(wg_ref.at[l], wgu.at[l, 0, pl.ds(mine, rows), :], load_sem.at[1 + 3 * l]),
            pltpu.make_async_copy(wu_ref.at[l], wgu.at[l, 1, pl.ds(mine, rows), :], load_sem.at[2 + 3 * l]),
            pltpu.make_async_copy(wd_ref.at[l], wdn.at[l, pl.ds(dmine, drows), :], load_sem.at[3 + 3 * l]),
        ]
    loads.append(pltpu.make_async_copy(dy_ref.at[0], g, load_sem.at[1 + 3 * layers]))
    for c in loads:
        c.start()

    barrier = pltpu.get_barrier_semaphore()
    for other in (*toward, {"rep": partner}, *({"rep": r} for r in across)):
        pl.semaphore_signal(barrier, inc=1, device_id=other, device_id_type=MESH)
    pl.semaphore_wait(barrier, 5)

    def axis(unit):
        return sum(divmod(unit, SEGMENTS + 1)) % 2

    def share(unit, other_core=False, other_side=False):
        c, side = 1 - core if other_core else core, sides[axis(unit)]
        return 2 * (1 - side if other_side else side) + c

    def piece(unit, direction, k, member):
        origin = at_distance(1 - direction, k)
        l, s = unit // (SEGMENTS + 1), unit % (SEGMENTS + 1)
        parts = 4
        halved = k == half
        if s < SEGMENTS:
            size, first, width = rows // parts, s * seg, seg
            if halved:
                width = seg // 2
                first += direction * width
            row = pl.multiple_of(origin * rows + member * size, size)
            return wgu.at[l, :, pl.ds(row, size), pl.ds(first, width)]
        size = drows // parts
        row = origin * drows + member * size
        if halved:
            size //= 2
            row += direction * size
        return wdn.at[l, pl.ds(pl.multiple_of(row, size), size), :]

    def ship(sems, unit, direction, k, ref, to):
        send, recv = sems
        return pltpu.make_async_remote_copy(
            ref, ref, send.at[unit, direction, k], recv.at[unit, direction, k], device_id=to, device_id_type=MESH
        )

    def hop(unit, direction, k):
        origin = at_distance(1 - direction, k)
        ref = piece(unit, direction, k, share(unit))
        if k == half - 1:
            ref = last_half(unit, direction, origin)
        return ship((ag_send, ag_recv), unit, direction, k, ref, toward[direction])

    def last_half(unit, direction, origin):
        l, s = unit // (SEGMENTS + 1), unit % (SEGMENTS + 1)
        parts, member = 4, share(unit)
        if s < SEGMENTS:
            size, width = rows // parts, seg // 2
            row = pl.multiple_of(origin * rows + member * size, size)
            return wgu.at[l, :, pl.ds(row, size), pl.ds(s * seg + direction * width, width)]
        size = drows // parts // 2
        row = origin * drows + (2 * member + direction) * size
        return wdn.at[l, pl.ds(pl.multiple_of(row, size), size), :]

    def landed(unit, direction, k):
        ref = piece(unit, direction, k + 1, share(unit))
        return ship((ag_send, ag_recv), unit, direction, k, ref, toward[direction])

    def swap(unit, direction, k, other_core=False):
        ref = piece(unit, direction, k + 1, share(unit, other_core))
        return ship((sw_send, sw_recv), unit, direction, k, ref, {"rep": partner})

    def cross(unit, direction, k, other_side=False):
        ref = piece(unit, direction, k + 1, share(unit, False, other_side))
        return ship((y_send, y_recv), unit, direction, k, ref, {"rep": across[axis(unit)]})

    def far(unit, direction, k, other_core=False):
        ref = piece(unit, direction, k + 1, share(unit, other_core, True))
        return ship((far_send, far_recv), unit, direction, k, ref, {"rep": partner})

    def gather(unit, k):
        for direction in range(2):
            if 0 < k <= half:
                landed(unit, direction, k - 1).wait_recv()
            if k < half:
                hop(unit, direction, k).start()
            if 0 < k <= half:
                cross(unit, direction, k - 1).start()
                swap(unit, direction, k - 1).start()
        if k > 1:
            for direction in range(2):
                cross(unit, direction, k - 2, True).wait_recv()
                far(unit, direction, k - 2).start()

    def gathered(unit):
        for k in range(half):
            for direction in range(2):
                swap(unit, direction, k, True).wait_recv()
                far(unit, direction, k, True).wait_recv()

    def close(unit):
        for k in range(half):
            for direction in range(2):
                hop(unit, direction, k).wait_send()
                swap(unit, direction, k).wait_send()
                cross(unit, direction, k).wait_send()
                far(unit, direction, k).wait_send()

    def place(u):
        step = jnp.minimum(u // per_layer, layers - 1)
        l = layers - 1 - step
        last = step == layers - 1
        first = jnp.where(last, 1, lead)
        v = u - step * per_layer
        r = v - first
        held = r - 2 * chunks
        even = lax.rem(jnp.maximum(r, 0), 2) == 0
        beside = last & even & (r >= 0) & (r < 2 * (subs - 1))
        down = (r < 0) | beside | ((held == 0) & jnp.logical_not(last))
        gate = jnp.logical_not(even) & (r > 0) & (held < 0)
        index = jnp.where(r < 0, v, jnp.where(held == 0, lead, jnp.where(beside, 1 + r // 2, r // 2)))
        slot = lax.rem(step * chunks + jnp.maximum(index, 0), SLOTS)
        base = jnp.where(down, dbase + l * ff + index * rows, slot * d_model)
        stride = jnp.where(down, drows, rows)
        return down | gate, l, down, index, base, stride

    def rs_copy(direction, k, u):
        lo, size = (direction * (rows // 2), rows // 2) if k == 0 else (0, rows)
        return pltpu.make_async_remote_copy(
            sbuf.at[direction, k, lax.rem(u, SEND), pl.ds(lo, size), :],
            rbuf.at[direction, k, lax.rem(u, RECV), pl.ds(lo, size), :],
            rs_send.at[direction, k, lax.rem(u, SEND)],
            rs_recv.at[direction, k, lax.rem(u, RECV)],
            device_id=toward[direction],
            device_id_type=MESH,
        )

    def stage(u, k, l, down, index, base, stride):
        hrows = rows // 2

        def own(owner, lo, size):
            return term[pl.ds(pl.multiple_of(base + owner * stride + lo, hrows), size), :]

        if k == half:
            for direction in range(2):
                rs_copy(direction, half - 1, u).wait_send()
                rs_copy(direction, half - 1, u).wait_recv()
            slot = lax.rem(u, RECV)
            total = own(me, 0, rows)
            for direction in range(2):
                total += rbuf[direction, half - 1, slot].astype(F32)
            total = total.astype(BF16)

            @pl.when(down)
            def _():
                outd[l, pl.ds(pl.multiple_of(index * rows, rows), rows), :] = total

            @pl.when(jnp.logical_not(down))
            def _():
                columns = pl.ds(pl.multiple_of(index * chunk, chunk), chunk)
                outg[l, :, columns] = total[:, :chunk]
                outu[l, :, columns] = total[:, chunk:]

            return
        for direction in range(2):
            owner = at_distance(direction, half - k)
            to = sbuf.at[direction, k, lax.rem(u, SEND)]
            lo = direction * hrows
            if k == 0:
                to[pl.ds(lo, hrows), :] = own(owner, lo, hrows).astype(BF16)
            else:
                rs_copy(direction, k - 1, u).wait_send()
                rs_copy(direction, k - 1, u).wait_recv()
                came = rbuf.at[direction, k - 1, lax.rem(u, RECV)]
                if k == 1:
                    rest = hrows - lo
                    to[pl.ds(lo, hrows), :] = (own(owner, lo, hrows) + came[pl.ds(lo, hrows), :].astype(F32)).astype(BF16)
                    to[pl.ds(rest, hrows), :] = own(owner, rest, hrows).astype(BF16)
                else:
                    to[...] = (own(owner, 0, rows) + came[...].astype(F32)).astype(BF16)
            rs_copy(direction, k, u).start()

    def tick(t):
        for k in range(half + 1):
            u = t - LAG * k
            there, *rest = place(jnp.maximum(u, 0))
            pl.when((u >= 0) & there)(functools.partial(stage, u, k, *rest))

    small, tile = min(256, tokens), min(512, tokens)

    def normed(l):
        @pl.loop(0, tokens // small)
        def _(i):
            ts = pl.ds(pl.multiple_of(i * small, small), small)
            wide = h[l, ts, :].astype(F32)
            scale = lax.rsqrt(jnp.mean(wide * wide, -1, keepdims=True) + 1e-6)
            rounded = (wide * scale).astype(BF16)
            a[ts, :] = rounded
            at[:, ts] = rounded.T

    def turn():
        @pl.loop(0, tokens // small)
        def _(i):
            ts = pl.ds(pl.multiple_of(i * small, small), small)
            gt[:, ts] = g[ts, :].T

    def both(l, columns):
        return jnp.concatenate([wgu[l, 0, :, columns], wgu[l, 1, :, columns]], 1)

    def forward(l, s, *between):
        @pl.loop(0, seg // chunk)
        def _(j):
            columns = pl.ds(pl.multiple_of(s * seg + j * chunk, chunk), chunk)
            w = both(l, columns)
            for i in range(tokens // tile):
                ts = pl.ds(i * tile, tile)
                out = dot(a[ts, :], w)
                gate, up = out[:, :chunk], out[:, chunk:]
                act[ts, columns] = (gate * jax.nn.sigmoid(gate) * up).astype(BF16)
            for number, steps in enumerate(between):
                if steps:
                    pl.when(j == number)(functools.partial(gathers, *steps))

    def down_forward(l):
        part = 2 * tile if tokens % (2 * tile) == 0 else tile

        @pl.loop(0, tokens // part)
        def _(i):
            for p in range(part // tile):
                ts = pl.ds(pl.multiple_of(i * part + p * tile, tile), tile)
                out = dot(act[ts, :], wdn[l]).astype(BF16)
                h[l + 1, ts, :] = (h[l, ts, :].astype(F32) + out.astype(F32)).astype(BF16)

    def down_gradient(l, start):
        @pl.loop(0, chunks // 2)
        def _(i):
            for p in range(2):
                j = 2 * i + p
                columns = pl.ds(pl.multiple_of(j * chunk, chunk), chunk)
                out = dot(gt[...], act[:, columns])
                term[pl.ds(pl.multiple_of(dbase + l * ff + j * chunk, chunk), chunk), :] = out.T
            if start > 0:
                pl.when(i == 1)(functools.partial(tick, start - 1))

    def backward_tokens(l, j):
        columns = pl.ds(pl.multiple_of(j * chunk, chunk), chunk)
        w, w_down = both(l, columns), wdn[l, columns, :]

        def first(i):
            ts = pl.ds(i * tile, tile)
            return dot(a[ts, :], w), dot_nt(g[ts, :], w_down)

        def second(i, out, by_act):
            ts = pl.ds(i * tile, tile)
            gate, up = out[:, :chunk], out[:, chunk:]
            by_act = by_act.astype(BF16).astype(F32)
            sig = jax.nn.sigmoid(gate)
            silu = gate * sig
            by_up = (by_act * silu).astype(BF16)
            by_gate = (by_act * up * (sig + silu * (1.0 - sig))).astype(BF16)
            by_both = jnp.concatenate([by_gate, by_up], 1)
            dgu[ts, :] = by_both
            da[ts, :] += dot_nt(by_both, w)

        tiles = tokens // tile
        ready = first(0)
        for i in range(1, tiles):
            after = first(i)
            second(i - 1, *ready)
            ready = after
        second(tiles - 1, *ready)

    def gate_up_gradient(step, j):
        row = pl.multiple_of(lax.rem(step * chunks + j, SLOTS) * d_model, d_model)
        term[pl.ds(row, d_model), :] = dot(at[...], dgu[...])

    def norm_backward(l):
        @pl.loop(0, tokens // small)
        def _(i):
            ts = pl.ds(pl.multiple_of(i * small, small), small)
            by_a = da[ts, :].astype(BF16).astype(F32)
            wide = h[l, ts, :].astype(F32)
            scale = lax.rsqrt(jnp.mean(wide * wide, -1, keepdims=True) + 1e-6)
            by_scale = jnp.sum(by_a * wide, -1, keepdims=True)
            by_wide = by_a * scale - (by_scale * scale / d_model) * (scale * scale) * wide
            g[ts, :] = (g[ts, :].astype(F32) + by_wide.astype(BF16).astype(F32)).astype(BF16)

    per = SEGMENTS + 1

    def gathers(*pairs):
        for unit, k in pairs:
            gather(unit, k)

    for c in loads[1:4]:
        c.wait()
    gathers((0, 0), (1, 0))
    loads[0].wait()
    normed(0)
    for c in loads[4:-1]:
        c.wait()
    gathers((2, 0), (3, 0), (0, 1), (1, 1), (2, 1), (3, 1), (0, 2), (1, 2), (2, 2), (3, 2), (0, 3), (4, 0), (1, 3))
    loads[-1].wait()
    turn()
    da[...] = jnp.zeros_like(da)
    gathers((2, 3), (5, 0), (3, 3), (0, 4), (4, 1), (1, 4), (2, 4), (5, 1), (0, 5), (3, 4))
    between = (
        (((1, 5), (4, 2)), (), ((2, 5), (5, 2)), ((3, 5),)),
        ((), ((4, 3),), (), ((5, 3),)),
        (((4, 4),), ((5, 4),), (), ((4, 5), (5, 5))),
        (),
    )
    keeps = []
    for l in range(layers):
        last = l + 1 == layers
        if l > 0:
            normed(l)
        for c in keeps:
            c.wait()
        keeps = []
        for i in range(SEGMENTS):
            gathered(l * per + i)
            forward(l, i, *between[l * SEGMENTS + i])
            if not last:
                columns = pl.ds(i * seg, seg)
                keeps.append(pltpu.make_async_copy(act.at[:, columns], kept.at[l, :, columns], keep_sem.at[i]))
                keeps[-1].start()
        gathered(l * per + SEGMENTS)
        if not last:
            down_forward(l)

    for step, l in enumerate(reversed(range(layers))):
        start = step * per_layer
        count = lead if l > 0 else 1
        if step > 0:
            da[...] = jnp.zeros_like(da)
            turn()
            normed(l)
            tick(start - 2)
            back.wait()
        down_gradient(l, start)
        if l > 0:
            back = pltpu.make_async_copy(kept.at[l - 1], act, keep_sem.at[SEGMENTS])
            back.start()

        @pl.loop(0, count)
        def _(i):
            tick(start + i)

        @pl.loop(0, chunks)
        def _(j):
            backward_tokens(l, j)
            tick(start + count + 2 * j)
            gate_up_gradient(step, j)
            tick(start + count + 1 + 2 * j)

        norm_backward(l)
        if l > 0:
            tick(start + count + 2 * chunks)

    out_dx = pltpu.make_async_copy(g, dx_ref.at[0], load_sem.at[0])
    out_dx.start()

    @pl.loop(0, LAG * half)
    def _(i):
        tick((layers - 1) * per_layer + 1 + 2 * chunks + i)

    outs = [
        pltpu.make_async_copy(outg, dwg_ref, load_sem.at[1]),
        pltpu.make_async_copy(outu, dwu_ref, load_sem.at[2]),
        pltpu.make_async_copy(outd, dwd_ref, load_sem.at[3]),
    ]
    for c in outs:
        c.start()
    for unit in range(layers * per):
        close(unit)
    for c in (out_dx, *outs):
        c.wait()


def solution(mesh):
    n = mesh.shape["dp"]

    def step(x, dy, wg, wu, wd):
        _, tokens, d_model = x.shape
        layers, rows, ff = wg.shape
        drows = wd.shape[1]
        chunk = d_model // 2
        half = n // 2
        gather_units = layers * (SEGMENTS + 1)
        any_space = pl.BlockSpec(memory_space=pl.ANY)
        dma = pltpu.SemaphoreType.DMA
        grads = pl.pallas_call(
            functools.partial(kernel, n, mesh.shape["rep"]),
            out_shape=[
                *(jax.ShapeDtypeStruct(t.shape, t.dtype) for t in (x, wg, wu, wd)),
                jax.ShapeDtypeStruct((layers - 1, tokens, ff), BF16),
            ],
            in_specs=[any_space] * 5,
            out_specs=[any_space] * 5,
            scratch_shapes=[
                pltpu.VMEM((layers, 2, d_model, ff), BF16),
                pltpu.VMEM((layers, ff, d_model), BF16),
                pltpu.VMEM((layers, tokens, d_model), BF16),
                pltpu.VMEM((tokens, d_model), BF16),
                pltpu.VMEM((d_model, tokens), BF16),
                pltpu.VMEM((tokens, d_model), BF16),
                pltpu.VMEM((d_model, tokens), BF16),
                pltpu.VMEM((tokens, ff), BF16),
                pltpu.VMEM((tokens, 2 * chunk), BF16),
                pltpu.VMEM((tokens, d_model), F32),
                pltpu.VMEM((SLOTS * d_model + layers * ff, d_model), F32),
                pltpu.VMEM((2, half, SEND, rows, d_model), BF16),
                pltpu.VMEM((2, half, RECV, rows, d_model), BF16),
                pltpu.VMEM((layers, rows, ff), BF16),
                pltpu.VMEM((layers, rows, ff), BF16),
                pltpu.VMEM((layers, drows, d_model), BF16),
                dma((2 + 3 * layers,)),
                dma((SEGMENTS + 1,)),
                dma((gather_units, 2, half)),
                dma((gather_units, 2, half)),
                dma((gather_units, 2, half)),
                dma((gather_units, 2, half)),
                dma((gather_units, 2, half)),
                dma((gather_units, 2, half)),
                dma((gather_units, 2, half)),
                dma((gather_units, 2, half)),
                dma((2, half, SEND)),
                dma((2, half, RECV)),
            ],
            compiler_params=pltpu.CompilerParams(
                collective_id=0, has_side_effects=True, vmem_limit_bytes=67043328
            ),
        )(x, dy, wg, wu, wd)[:4]
        steps = 4

        def settle(*refs):
            for source, to in zip(refs[:4], refs[4:]):
                to[...] = source[...]

        blocks = [
            pl.BlockSpec((t.shape[0], t.shape[1] // steps, t.shape[2]), lambda i: (0, i, 0)) for t in grads
        ]
        return pl.pallas_call(
            settle,
            grid=(steps,),
            in_specs=blocks,
            out_specs=blocks,
            out_shape=[jax.ShapeDtypeStruct(t.shape, t.dtype) for t in grads],
        )(*grads)

    tokens_spec, weight_spec = P(("rep", "dp"), None, None), P(None, "dp", None)
    grad_spec = P("rep", "dp", None)
    return jax.shard_map(
        step,
        mesh=mesh,
        in_specs=(tokens_spec, tokens_spec, weight_spec, weight_spec, weight_spec),
        out_specs=(tokens_spec, grad_spec, grad_spec, grad_spec),
        check_vma=False,
    )
```
